128 devices in a mesh: gz: 64 (over z, y, x_lo, core), ba: 2 (over x_hi).
Axes of the slice: x: 4 (x_hi: 2, x_lo: 2; x = x_hi * 2 + x_lo), y: 4, z: 4, core: 2. Of those that a mesh axis runs over, the one named last changes fastest.
Arguments:
- coeffs: float32 [2, 3, 4, 128, 128, 128], P(None, None, 'ba', 'gz'), may hold values from -6 to 6
- material: int32 [128, 128, 128], P('gz'), may hold values from 0 to 3
- inv_diag: float32 [4, 3], replicated, may hold values from 0.1 to 1
- inv_off: float32 [4, 3], replicated, may hold values from -0.1 to 0.1
Outputs:
- theta: float32 [2, 3, 4, 128, 128, 128], P(None, None, 'ba', 'gz')
- gram: float32 [2, 4, 4], P(None, None, 'ba')
The draws below stay inside these ranges and needn't reach their ends.
Inputs may be any that keep to these rules, and one draw needn't show every extreme that they name: material indices.
All inputs are finite; a program needn't handle non-finite values.
Results may differ from the reference program's by a relative error of at most 0.00011.
Values sent between devices are 32-bit elements; how exact they have to be, the bound alone decides.
A program may use at most 64 MiB of HBM per device.

```python
import math
import jax
import jax.numpy as jnp
from jax import lax

NX = 128
NY = 128
CZ = 2
MATERIALS = 4
NZ = 128
BANDS = 4
N_GZ = 64


def with_ends(values, stream_key, low, largest):
    index_at = [jax.random.randint(jax.random.fold_in(stream_key, axis), (), 0, length) for axis, length in enumerate(values.shape)]
    widest = values.shape.index(max(values.shape))
    next_to = index_at[:widest] + [(index_at[widest] + 1) % values.shape[widest]] + index_at[widest + 1:]
    return values.at[tuple(index_at)].set(low).at[tuple(next_to)].set(largest)


def block_levels(rng, extent, cuts, low, largest):
    def one(axis_at, blocks):
        heights = jax.random.uniform(jax.random.fold_in(jax.random.fold_in(rng, 6), axis_at), (blocks,), jnp.float32, low / len(cuts), largest / len(cuts))
        return jnp.repeat(jnp.exp(heights), extent[axis_at] // blocks).reshape((-1,) + (1,) * (len(extent) - axis_at - 1))

    factor_of = one(*cuts[0])
    for cut in cuts[1:]:
        factor_of = factor_of * one(*cut)
    return factor_of


def noise(key, extent, width, reach, cuts=(), kind=jnp.bfloat16):
    entries = jax.random.normal(key, extent, jnp.float32) * width
    if len(cuts) > 0:
        entries = block_levels(key, extent, cuts, -0.22, 0.18) * entries
    return jnp.clip(entries, min=-reach, max=reach).astype(kind)


def setup_inputs(seed: int = 0) -> dict:
    streams_of = jax.random.split(jax.random.key(seed), 5)
    return {
        "coeffs": noise(streams_of[0], (2, 3, BANDS, NZ, NY, NX), 1.0, 6.0, ((2, 2), (3, 64)), jnp.float32),
        "material": with_ends(jax.random.randint(streams_of[1], (NZ, NY, NX), 0, MATERIALS), jax.random.fold_in(streams_of[1], 1), 0, MATERIALS - 1).astype(jnp.int32),
        "inv_diag": jnp.clip(jnp.exp(jax.random.uniform(streams_of[2], (MATERIALS, 3), jnp.float32, math.log(0.1), math.log(1.0))), 0.1, 1.0),
        "inv_off": jnp.clip(jax.random.uniform(streams_of[3], (MATERIALS, 3), jnp.float32, -0.1, 0.1), -0.1, 0.1),
    }


highest = lax.Precision.HIGHEST


def reverse_bits(values, levels):
    flipped = jnp.zeros_like(values)
    for position in range(levels):
        flipped = flipped + ((values >> position) & 1) * (1 << (levels - 1 - position))
    return flipped


def signed_wave(numbers, length):
    shifted = jnp.where(numbers < length // 2, numbers, numbers - length)
    return shifted.astype(jnp.float32) / (length / 2.0)


def cross_waves(waves, field):
    first, second, third = waves
    return jnp.stack([second * field[2] - third * field[1],
                      third * field[0] - first * field[2],
                      first * field[1] - second * field[0]])


def reference(coeffs, material, inv_diag, inv_off):
    levels = N_GZ.bit_length() - 1
    rows = jnp.arange(NZ, dtype=jnp.int32)
    wave_rows = reverse_bits(rows // CZ, levels) + N_GZ * (rows % CZ)
    natural = jnp.zeros((NZ,), jnp.int32).at[wave_rows].set(rows)
    waves = (signed_wave(jnp.arange(NX, dtype=jnp.int32), NX)[None, None, :],
             signed_wave(jnp.arange(NY, dtype=jnp.int32), NY)[None, :, None],
             signed_wave(wave_rows, NZ)[:, None, None])
    onehot = (material[None] == jnp.arange(MATERIALS, dtype=jnp.int32)[:, None, None, None]).astype(jnp.float32)
    table = jnp.concatenate([inv_diag, inv_off], axis=1)
    tensor = jnp.einsum("mk,mzyx->kzyx", table, onehot, precision=highest)

    def one_band(band):
        spectral = band[0] + 1j * band[1]
        curl = cross_waves(waves, spectral)[:, natural]
        field = jnp.fft.ifftn(curl, axes=(1, 2, 3), norm="ortho")
        scaled = jnp.stack([tensor[0] * field[0] + tensor[3] * field[1] + tensor[5] * field[2],
                            tensor[3] * field[0] + tensor[1] * field[1] + tensor[4] * field[2],
                            tensor[5] * field[0] + tensor[4] * field[1] + tensor[2] * field[2]])
        back = jnp.fft.fftn(scaled, axes=(1, 2, 3), norm="ortho")[:, wave_rows]
        result = -cross_waves(waves, back)
        return jnp.stack([jnp.real(result), jnp.imag(result)]).astype(jnp.float32)

    theta = jnp.moveaxis(lax.map(one_band, jnp.moveaxis(coeffs, 2, 0)), 0, 2)
    factor = 1.0 / (NX * NY * NZ)
    real_part = (jnp.einsum("cbzyx,cezyx->be", coeffs[0], theta[0], precision=highest)
                 + jnp.einsum("cbzyx,cezyx->be", coeffs[1], theta[1], precision=highest)) * factor
    imag_part = (jnp.einsum("cbzyx,cezyx->be", coeffs[0], theta[1], precision=highest)
                 - jnp.einsum("cbzyx,cezyx->be", coeffs[1], theta[0], precision=highest)) * factor
    gram = jnp.stack([real_part, imag_part])
    return theta, gram
```

```python
import jax
import jax.numpy as jnp
import numpy as np
from jax import lax
from jax.experimental import pallas as pl
from jax.experimental.pallas import tpu as pltpu
from jax.sharding import PartitionSpec as P

LOGICAL = pl.DeviceIdType.LOGICAL
N = 128
GZ = 64
DEV = 128
CHUNKS = 3


def reverse_bits_np(values, levels):
    flipped = np.zeros_like(values)
    for position in range(levels):
        flipped = flipped + ((values >> position) & 1) * (1 << (levels - 1 - position))
    return flipped


def as_parts(table):
    high = table.astype(jnp.bfloat16)
    low = (table - high.astype(np.float64)).astype(jnp.bfloat16)
    return np.stack([high, low])


def tables():
    index = np.arange(N)
    scale = 1.0 / np.sqrt(N)
    angle = 2.0 * np.pi / N * (index[:, None] * index[None, :] % N)
    cosine, sine = np.cos(angle) * scale, np.sin(angle) * scale
    first = np.block([[cosine, sine], [-sine, cosine]])
    second = np.block([[cosine, -sine], [sine, cosine]])
    device = np.arange(GZ)
    planes = np.concatenate([device * 2, device * 2 + 1])
    reversed_device = reverse_bits_np(device, 6)
    numbers = np.concatenate([reversed_device, reversed_device + GZ])
    angle = 2.0 * np.pi / N * (planes[:, None] * numbers[None, :] % N)
    cosine, sine = np.cos(angle) * scale, np.sin(angle) * scale
    inverse = np.block([[cosine, -sine], [sine, cosine]])
    return np.stack([as_parts(t) for t in (first, second, inverse, inverse.T)])


def split(values):
    high = values.astype(jnp.bfloat16)
    low = (values - high.astype(jnp.float32)).astype(jnp.bfloat16)
    return high, low


def dot(left, right):
    return jnp.dot(left, right, preferred_element_type=jnp.float32)


def times_table(data, table_ref, which):
    high, low = split(data)
    return dot(high, table_ref[which, 0]) + (dot(low, table_ref[which, 0]) + dot(high, table_ref[which, 1]))


def table_times(table_ref, which, data):
    high, low = split(data)
    return dot(table_ref[which, 0], high) + (dot(table_ref[which, 0], low) + dot(table_ref[which, 1], high))


def swap_blocks(values):
    top = jnp.concatenate([values[:N, :N], values[N:, :N]], axis=1)
    bottom = jnp.concatenate([values[:N, N:], values[N:, N:]], axis=1)
    return jnp.concatenate([top, bottom], axis=0)


def kernel(
    coeffs_hbm, material_hbm, diag_ref, off_ref, tables_hbm,
    theta_hbm, gram_ref,
    coeffs, material, table, work, send1, recv1, field, scaled, send2, recv2, theta,
    material_send, material_recv, gram_send, gram_recv,
    in_sem, out_sem, send_sem, recv_sem,
):
    gz = lax.axis_index("gz")
    ba = lax.axis_index("ba")
    me = gz * 2 + ba
    mine = ba * GZ + gz

    barrier = pltpu.get_barrier_semaphore()

    def greet(i, carry):
        pl.semaphore_signal(barrier, inc=1, device_id=lax.rem(me + 1 + i, DEV), device_id_type=LOGICAL)
        return carry

    loads = [
        pltpu.make_async_copy(coeffs_hbm.at[:, :, band], coeffs.at[band], in_sem.at[band]) for band in range(2)
    ]
    table_load = pltpu.make_async_copy(tables_hbm, table, in_sem.at[2])
    material_load = pltpu.make_async_copy(material_hbm, material, in_sem.at[3])
    loads[0].start()
    table_load.start()
    loads[1].start()
    material_load.start()
    lax.fori_loop(0, DEV - 1, greet, 0, unroll=4)

    qx = lax.broadcasted_iota(jnp.int32, (N, N), 1)
    qx = jnp.where(qx < N // 2, qx, qx - N).astype(jnp.float32) * (1.0 / (N // 2))
    qy = lax.broadcasted_iota(jnp.int32, (N, N), 0)
    qy = jnp.where(qy < N // 2, qy, qy - N).astype(jnp.float32) * (1.0 / (N // 2))
    flipped = 0
    rest = gz
    for _ in range(6):
        flipped = flipped * 2 + lax.rem(rest, 2)
        rest = lax.div(rest, 2)
    qz = [flipped.astype(jnp.float32) * (1.0 / (N // 2)), (flipped - N // 2).astype(jnp.float32) * (1.0 / (N // 2))]

    def curl_of(get, put, sign):
        for plane in range(2):
            for part in range(2):
                hx, hy, hz = get(0, plane, part), get(1, plane, part), get(2, plane, part)
                if sign > 0:
                    put(0, plane, part, qy * hz - qz[plane] * hy)
                    put(1, plane, part, qz[plane] * hx - qx * hz)
                    put(2, plane, part, qx * hy - qy * hx)
                else:
                    put(0, plane, part, qz[plane] * hy - qy * hz)
                    put(1, plane, part, qx * hz - qz[plane] * hx)
                    put(2, plane, part, qy * hx - qx * hy)

    def block(plane, part):
        return pl.ds(plane * N, N), pl.ds(part * N, N)

    def spread(chunk, source, target, base):
        def one(i, carry):
            to = lax.rem(me + 1 + i, DEV)
            row = lax.rem(to, 2) * GZ + lax.div(to, 2)
            pltpu.make_async_remote_copy(
                src_ref=source.at[chunk, pl.ds(pl.multiple_of(row * 8, 8), 8)],
                dst_ref=target.at[chunk, pl.ds(pl.multiple_of(mine * 8, 8), 8)],
                send_sem=send_sem.at[base + chunk],
                recv_sem=recv_sem.at[base + chunk],
                device_id=to,
                device_id_type=LOGICAL,
            ).start()
            return carry

        lax.fori_loop(0, DEV - 1, one, 0, unroll=4)
        own = pl.ds(pl.multiple_of(mine * 8, 8), 8)
        target[chunk, own, :] = source[chunk, own, :]

    def chunk_of_others(ref, sem):
        rows = (DEV - 1) * 8
        return pltpu.make_async_copy(ref.at[0, pl.ds(0, rows)], ref.at[0, pl.ds(0, rows)], sem)

    def forward_xy(q):
        plane_rows = times_table(work[q], table, 0)
        out = table_times(table, 1, swap_blocks(plane_rows))
        for part in range(2):
            for plane in range(2):
                row = (q % 2) * 4 + part * 2 + plane
                send1[q // 2, pl.ds(row, N, stride=8), :] = out[part * N : (part + 1) * N, plane * N : (plane + 1) * N]

    def curl_in(band):
        def get(c, plane, part):
            return coeffs[band, part, c, plane]

        def put(c, plane, part, value):
            rows, lanes = block(plane, part)
            work[band * 3 + c, rows, lanes] = value

        curl_of(get, put, 1)

    loads[0].wait()
    curl_in(0)
    table_load.wait()
    forward_xy(0)
    forward_xy(1)
    pl.semaphore_wait(barrier, DEV - 1)
    spread(0, send1, recv1, 0)

    material_load.wait()
    for plane in range(2):
        material_send[:, plane, :] = material[plane]

    def material_to(i, carry):
        to = lax.rem(gz + 1 + i, GZ)
        pltpu.make_async_remote_copy(
            src_ref=material_send.at[ba * GZ + to],
            dst_ref=material_recv.at[gz],
            send_sem=send_sem.at[6],
            recv_sem=recv_sem.at[6],
            device_id=to * 2 + ba,
            device_id_type=LOGICAL,
        ).start()
        return carry

    lax.fori_loop(0, GZ - 1, material_to, 0, unroll=4)
    material_recv[gz] = material_send[mine]

    loads[1].wait()
    curl_in(1)
    forward_xy(2)
    forward_xy(3)
    spread(1, send1, recv1, 0)
    forward_xy(4)
    forward_xy(5)
    spread(2, send1, recv1, 0)

    def inverse_z(q):
        lines = []
        for part in range(2):
            for plane in range(2):
                row = (q % 2) * 4 + part * 2 + plane
                lines.append(
                    jnp.concatenate(
                        [recv1[q // 2, pl.ds(group * GZ * 8 + row, GZ, stride=8), :] for group in range(2)], axis=1
                    )
                )
        field[q] = table_times(table, 2, jnp.concatenate(lines, axis=0))

    def forward_z(q):
        out = table_times(table, 3, scaled[q])
        for part in range(2):
            for plane in range(2):
                row = (q % 2) * 4 + part * 2 + plane
                start = (part * 2 + plane) * GZ
                for group in range(2):
                    send2[q // 2, pl.ds(group * GZ * 8 + row, GZ, stride=8), :] = out[
                        start : start + GZ, group * N : (group + 1) * N
                    ]

    def entry(k, index):
        ref, column = (diag_ref, k) if k < 3 else (off_ref, k - 3)
        value = jnp.where(index == 1, ref[1, column], ref[0, column])
        value = jnp.where(index == 2, ref[2, column], value)
        return jnp.where(index == 3, ref[3, column], value)

    def apply_material(band):
        for half in range(2):
            index = material_recv[:, half, :]
            xx, yy, zz, xy, yz, zx = [entry(k, index) for k in range(6)]
            for part in range(2):
                for group in range(2):
                    rows, lanes = pl.ds(part * N + half * GZ, GZ), pl.ds(group * N, N)
                    fx, fy, fz = [field[band * 3 + c, rows, lanes] for c in range(3)]
                    scaled[band * 3, rows, lanes] = xx * fx + xy * fy + zx * fz
                    scaled[band * 3 + 1, rows, lanes] = xy * fx + yy * fy + yz * fz
                    scaled[band * 3 + 2, rows, lanes] = zx * fx + yz * fy + zz * fz

    chunk_of_others(recv1, recv_sem.at[0]).wait()
    inverse_z(0)
    inverse_z(1)
    pltpu.make_async_copy(
        material_recv.at[pl.ds(0, GZ - 1)], material_recv.at[pl.ds(0, GZ - 1)], recv_sem.at[6]
    ).wait()
    chunk_of_others(recv1, recv_sem.at[1]).wait()
    inverse_z(2)
    apply_material(0)
    forward_z(0)
    forward_z(1)
    spread(0, send2, recv2, 3)
    forward_z(2)
    inverse_z(3)
    chunk_of_others(recv1, recv_sem.at[2]).wait()
    inverse_z(4)
    inverse_z(5)
    apply_material(1)
    forward_z(3)
    spread(1, send2, recv2, 3)
    forward_z(4)
    forward_z(5)
    spread(2, send2, recv2, 3)

    def gram_step(i, sums):
        sums = list(sums)
        for c in range(3):
            values = []
            for ref in (field, scaled):
                values.append(
                    [
                        [
                            ref[(e % 2) * 3 + c, pl.ds(pl.multiple_of(part * N + i * 8, 8), 8), pl.ds((e // 2) * N, N)]
                            for part in range(2)
                        ]
                        for e in range(4)
                    ]
                )
            f, s = values
            for a in range(4):
                for e in range(4):
                    k = a * 4 + e
                    sums[k] = sums[k] + (f[a][0] * s[e][0] + f[a][1] * s[e][1])
                    sums[16 + k] = sums[16 + k] + (f[a][0] * s[e][1] - f[a][1] * s[e][0])
        return tuple(sums)

    sums = lax.fori_loop(0, N // 8, gram_step, tuple(jnp.zeros((8, N), jnp.float32) for _ in range(32)))
    lane = lax.broadcasted_iota(jnp.int32, (1, N), 1)
    packed = jnp.zeros((1, N), jnp.float32)
    for k in range(32):
        total = jnp.sum(jnp.sum(sums[k], axis=0, keepdims=True), axis=1, keepdims=True)
        packed = packed + jnp.where(lane == k, total, 0.0)
    gram_send[0] = packed
    gram_recv[mine] = packed

    def gram_to(i, carry):
        pltpu.make_async_remote_copy(
            src_ref=gram_send.at[0],
            dst_ref=gram_recv.at[mine],
            send_sem=send_sem.at[7],
            recv_sem=recv_sem.at[7],
            device_id=lax.rem(me + 1 + i, DEV),
            device_id_type=LOGICAL,
        ).start()
        return carry

    lax.fori_loop(0, DEV - 1, gram_to, 0, unroll=4)

    def forward_yx(q):
        halves = []
        for part in range(2):
            halves.append(
                jnp.concatenate(
                    [
                        recv2[q // 2, pl.ds((q % 2) * 4 + part * 2 + plane, N, stride=8), :]
                        for plane in range(2)
                    ],
                    axis=1,
                )
            )
        columns = table_times(table, 0, jnp.concatenate(halves, axis=0))
        work[q] = times_table(swap_blocks(columns), table, 1)

    def curl_out(band):
        def get(c, plane, part):
            rows, lanes = block(plane, part)
            return work[band * 3 + c, rows, lanes]

        def put(c, plane, part, value):
            theta[band, part, c, plane] = value

        curl_of(get, put, -1)

    stores = [
        pltpu.make_async_copy(theta.at[band], theta_hbm.at[:, :, band], out_sem.at[band]) for band in range(2)
    ]
    chunk_of_others(recv2, recv_sem.at[3]).wait()
    forward_yx(0)
    forward_yx(1)
    chunk_of_others(recv2, recv_sem.at[4]).wait()
    forward_yx(2)
    curl_out(0)
    stores[0].start()
    forward_yx(3)
    chunk_of_others(recv2, recv_sem.at[5]).wait()
    forward_yx(4)
    forward_yx(5)
    curl_out(1)
    stores[1].start()

    pltpu.make_async_copy(gram_recv.at[pl.ds(0, DEV - 1)], gram_recv.at[pl.ds(0, DEV - 1)], recv_sem.at[7]).wait()
    whole = jnp.sum(gram_recv[...], axis=0) * (1.0 / (N * N * N))
    across = lax.broadcasted_iota(jnp.int32, (8, N), 1)
    row = lax.broadcasted_iota(jnp.int32, (8, N), 0)
    columns = [
        jnp.sum(jnp.where(across == row * 4 + (ba * 2 + e), whole, 0.0), axis=1, keepdims=True) for e in range(2)
    ]
    gram = jnp.concatenate(columns, axis=1)
    gram_ref[0] = gram[:4]
    gram_ref[1] = gram[4:]

    for chunk in range(CHUNKS):
        chunk_of_others(send1, send_sem.at[chunk]).wait()
        chunk_of_others(send2, send_sem.at[3 + chunk]).wait()
    pltpu.make_async_copy(
        material_send.at[pl.ds(0, GZ - 1)], material_send.at[pl.ds(0, GZ - 1)], send_sem.at[6]
    ).wait()
    pltpu.make_async_copy(gram_recv.at[pl.ds(0, DEV - 1)], gram_recv.at[pl.ds(0, DEV - 1)], send_sem.at[7]).wait()
    stores[0].wait()
    stores[1].wait()


def on_device(coeffs, material, inv_diag, inv_off):
    f32 = jnp.float32
    anywhere = pl.BlockSpec(memory_space=pl.ANY)
    smem = pl.BlockSpec(memory_space=pltpu.SMEM)
    theta, gram = pl.pallas_call(
        kernel,
        out_shape=(jax.ShapeDtypeStruct(coeffs.shape, f32), jax.ShapeDtypeStruct((2, 4, 2), f32)),
        in_specs=[anywhere, anywhere, smem, smem, anywhere],
        out_specs=(anywhere, pl.BlockSpec(memory_space=pltpu.VMEM)),
        scratch_shapes=[
            pltpu.VMEM((2, 2, 3, 2, N, N), f32),
            pltpu.VMEM((2, N, N), jnp.int32),
            pltpu.VMEM((4, 2, 2 * N, 2 * N), jnp.bfloat16),
            pltpu.VMEM((6, 2 * N, 2 * N), f32),
            pltpu.VMEM((CHUNKS, DEV * 8, N), f32),
            pltpu.VMEM((CHUNKS, DEV * 8, N), f32),
            pltpu.VMEM((6, 2 * N, 2 * N), f32),
            pltpu.VMEM((6, 2 * N, 2 * N), f32),
            pltpu.VMEM((CHUNKS, DEV * 8, N), f32),
            pltpu.VMEM((CHUNKS, DEV * 8, N), f32),
            pltpu.VMEM((2, 2, 3, 2, N, N), f32),
            pltpu.VMEM((DEV, 2, N), jnp.int32),
            pltpu.VMEM((GZ, 2, N), jnp.int32),
            pltpu.VMEM((1, 1, N), f32),
            pltpu.VMEM((DEV, 1, N), f32),
            pltpu.SemaphoreType.DMA((4,)),
            pltpu.SemaphoreType.DMA((2,)),
            pltpu.SemaphoreType.DMA((8,)),
            pltpu.SemaphoreType.DMA((8,)),
        ],
        compiler_params=pltpu.CompilerParams(collective_id=0, has_side_effects=True),
        name="maxwell",
    )(coeffs, material, inv_diag, inv_off, jnp.asarray(tables()))
    return theta, gram


def solution(mesh):
    in_specs = (P(None, None, "ba", "gz", None, None), P("gz", None, None), P(), P())
    out_specs = (P(None, None, "ba", "gz", None, None), P(None, None, "ba"))
    return jax.shard_map(
        on_device, mesh=mesh, in_specs=in_specs, out_specs=out_specs, check_vma=False
    )
```

```python
import jax
import jax.numpy as jnp
import numpy as np
from jax import lax
from jax.experimental import pallas as pl
from jax.experimental.pallas import tpu as pltpu
from jax.sharding import PartitionSpec as P

LOGICAL = pl.DeviceIdType.LOGICAL
N = 128
GZ = 64
DEV = 128
CHUNKS = 3


def reverse_bits_np(values, levels):
    flipped = np.zeros_like(values)
    for position in range(levels):
        flipped = flipped + ((values >> position) & 1) * (1 << (levels - 1 - position))
    return flipped


def as_parts(table):
    high = table.astype(jnp.bfloat16)
    low = (table - high.astype(np.float64)).astype(jnp.bfloat16)
    return np.stack([high, low])


def tables():
    index = np.arange(N)
    scale = 1.0 / np.sqrt(N)
    angle = 2.0 * np.pi / N * (index[:, None] * index[None, :] % N)
    cosine, sine = np.cos(angle) * scale, np.sin(angle) * scale
    first = np.block([[cosine, sine], [-sine, cosine]])
    second = np.block([[cosine, -sine], [sine, cosine]])
    device = np.arange(GZ)
    planes = np.concatenate([device * 2, device * 2 + 1])
    reversed_device = reverse_bits_np(device, 6)
    numbers = np.concatenate([reversed_device, reversed_device + GZ])
    angle = 2.0 * np.pi / N * (planes[:, None] * numbers[None, :] % N)
    cosine, sine = np.cos(angle) * scale, np.sin(angle) * scale
    inverse = np.block([[cosine, -sine], [sine, cosine]])
    return np.stack([as_parts(t) for t in (first, second, inverse, inverse.T)])


def split(values):
    high = values.astype(jnp.bfloat16)
    low = (values - high.astype(jnp.float32)).astype(jnp.bfloat16)
    return high, low


def dot(left, right):
    return jnp.dot(left, right, preferred_element_type=jnp.float32)


def times_table(data, table_ref, which):
    high, low = split(data)
    return dot(high, table_ref[which, 0]) + (dot(low, table_ref[which, 0]) + dot(high, table_ref[which, 1]))


def table_times(table_ref, which, data):
    high, low = split(data)
    return dot(table_ref[which, 0], high) + (dot(table_ref[which, 0], low) + dot(table_ref[which, 1], high))


def swap_blocks(values):
    top = jnp.concatenate([values[:N, :N], values[N:, :N]], axis=1)
    bottom = jnp.concatenate([values[:N, N:], values[N:, N:]], axis=1)
    return jnp.concatenate([top, bottom], axis=0)


def wavevectors(gz):
    qx = lax.broadcasted_iota(jnp.int32, (N, N), 1)
    qx = jnp.where(qx < N // 2, qx, qx - N).astype(jnp.float32) * (1.0 / (N // 2))
    qy = lax.broadcasted_iota(jnp.int32, (N, N), 0)
    qy = jnp.where(qy < N // 2, qy, qy - N).astype(jnp.float32) * (1.0 / (N // 2))
    flipped = 0
    rest = gz
    for _ in range(6):
        flipped = flipped * 2 + lax.rem(rest, 2)
        rest = lax.div(rest, 2)
    qz = [flipped.astype(jnp.float32) * (1.0 / (N // 2)), (flipped - N // 2).astype(jnp.float32) * (1.0 / (N // 2))]
    return qx, qy, qz


def block(plane, part):
    return pl.ds(plane * N, N), pl.ds(part * N, N)


def kernel(
    coeffs_hbm, material_hbm, diag_ref, off_ref, tables_hbm,
    work, sums_ref,
    coeffs, material, table, send1, recv1, field, scaled, send2, recv2,
    material_send, material_recv, tensor, gram_send, gram_recv,
    in_sem, send_sem, recv_sem, group_sem,
):
    gz = lax.axis_index("gz")
    ba = lax.axis_index("ba")
    me = gz * 2 + ba
    mine = ba * GZ + gz

    line, place = lax.div(me, 8), lax.rem(me, 8)
    barrier = pltpu.get_barrier_semaphore()
    places = [lax.rem(place + i, 8) for i in range(8)]
    rows_of = [lax.rem(p, 2) * GZ + lax.div(p, 2) for p in places]

    def line_at(i):
        return lax.rem(line + i, 16)

    for i in range(1, 16):
        pl.semaphore_signal(barrier, inc=1, device_id=line_at(i) * 8 + place, device_id_type=LOGICAL)
    for i in range(1, 8):
        pl.semaphore_signal(barrier, inc=1, device_id=line * 8 + places[i], device_id_type=LOGICAL)

    loads = [
        pltpu.make_async_copy(coeffs_hbm.at[:, :, band], coeffs.at[band], in_sem.at[band]) for band in range(2)
    ]
    table_load = pltpu.make_async_copy(tables_hbm, table, in_sem.at[2])
    material_load = pltpu.make_async_copy(material_hbm, material, in_sem.at[3])
    loads[0].start()
    table_load.start()
    loads[1].start()
    material_load.start()

    qx, qy, qz = wavevectors(gz)

    def to_known(send):
        def one(i, carry):
            there = line_at(i)
            send(there * 8 + place, there * 4 + rows_of[0])
            return carry

        lax.fori_loop(1, 16, one, 0, unroll=5)
        for i in range(1, 8):
            send(line * 8 + places[i], line * 4 + rows_of[i])

    def to_rest(send):
        def one(i, carry):
            there = line_at(i)
            for k in range(1, 8):
                send(there * 8 + places[k], there * 4 + rows_of[k])
            return carry

        lax.fori_loop(1, 16, one, 0)

    def piece(chunk, source, target, base):
        def send(to, row):
            pltpu.make_async_remote_copy(
                src_ref=source.at[chunk, pl.ds(pl.multiple_of(row * 8, 8), 8)],
                dst_ref=target.at[chunk, pl.ds(pl.multiple_of(mine * 8, 8), 8)],
                send_sem=send_sem.at[base + chunk],
                recv_sem=recv_sem.at[base + chunk],
                device_id=to,
                device_id_type=LOGICAL,
            ).start()

        return send

    def keep(chunk, source, target):
        own = pl.ds(pl.multiple_of(mine * 8, 8), 8)
        target[chunk, own, :] = source[chunk, own, :]

    def spread(chunk, source, target, base):
        send = piece(chunk, source, target, base)
        to_known(send)
        to_rest(send)
        keep(chunk, source, target)

    def chunk_of_others(ref, sem):
        rows = (DEV - 1) * 8
        return pltpu.make_async_copy(ref.at[0, pl.ds(0, rows)], ref.at[0, pl.ds(0, rows)], sem)

    def forward_xy(*qs):
        rows = times_table(jnp.concatenate([work[q] for q in qs], axis=0), table, 0)
        blocks = [swap_blocks(rows[i * 2 * N : (i + 1) * 2 * N]) for i in range(len(qs))]
        out = table_times(table, 1, jnp.concatenate(blocks, axis=1))
        for i, q in enumerate(qs):
            for part in range(2):
                for plane in range(2):
                    row = (q % 2) * 4 + part * 2 + plane
                    start = i * 2 * N + plane * N
                    send1[q // 2, pl.ds(row, N, stride=8), :] = out[part * N : (part + 1) * N, start : start + N]

    def curl_in(band):
        for plane in range(2):
            for part in range(2):
                hx, hy, hz = [coeffs[band, part, c, plane] for c in range(3)]
                rows, lanes = block(plane, part)
                work[band * 3, rows, lanes] = qy * hz - qz[plane] * hy
                work[band * 3 + 1, rows, lanes] = qz[plane] * hx - qx * hz
                work[band * 3 + 2, rows, lanes] = qx * hy - qy * hx

    loads[0].wait()
    curl_in(0)
    table_load.wait()
    forward_xy(0, 1)
    pl.semaphore_wait(barrier, 22)
    for i in range(1, 8):
        pl.semaphore_signal(group_sem, inc=1, device_id=line * 8 + places[i], device_id_type=LOGICAL)
    to_known(piece(0, send1, recv1, 0))
    loads[1].wait()
    curl_in(1)
    material_load.wait()
    for plane in range(2):
        material_send[:, plane, :] = material[plane]
    forward_xy(2, 3)
    pl.semaphore_wait(group_sem, 7)
    to_rest(piece(0, send1, recv1, 0))
    keep(0, send1, recv1)

    def material_to(i, carry):
        to = lax.rem(gz + i, GZ)
        pltpu.make_async_remote_copy(
            src_ref=material_send.at[ba * GZ + to],
            dst_ref=material_recv.at[gz],
            send_sem=send_sem.at[6],
            recv_sem=recv_sem.at[6],
            device_id=to * 2 + ba,
            device_id_type=LOGICAL,
        ).start()
        return carry

    lax.fori_loop(1, GZ, material_to, 0, unroll=7)
    material_recv[gz] = material_send[mine]
    spread(1, send1, recv1, 0)
    forward_xy(4, 5)

    def inverse_z(*qs):
        columns = []
        for q in qs:
            lines = []
            for part in range(2):
                for plane in range(2):
                    row = (q % 2) * 4 + part * 2 + plane
                    lines.append(
                        jnp.concatenate(
                            [recv1[q // 2, pl.ds(group * GZ * 8 + row, GZ, stride=8), :] for group in range(2)],
                            axis=1,
                        )
                    )
            columns.append(jnp.concatenate(lines, axis=0))
        out = table_times(table, 2, jnp.concatenate(columns, axis=1))
        for i, q in enumerate(qs):
            field[q] = out[:, i * 2 * N : (i + 1) * 2 * N]

    def forward_z(*qs):
        out = table_times(table, 3, jnp.concatenate([scaled[q] for q in qs], axis=1))
        for i, q in enumerate(qs):
            for part in range(2):
                for plane in range(2):
                    row = (q % 2) * 4 + part * 2 + plane
                    start = (part * 2 + plane) * GZ
                    for group in range(2):
                        lanes = i * 2 * N + group * N
                        send2[q // 2, pl.ds(group * GZ * 8 + row, GZ, stride=8), :] = out[
                            start : start + GZ, lanes : lanes + N
                        ]

    def entry(k, index):
        ref, column = (diag_ref, k) if k < 3 else (off_ref, k - 3)
        value = jnp.where(index == 1, ref[1, column], ref[0, column])
        value = jnp.where(index == 2, ref[2, column], value)
        return jnp.where(index == 3, ref[3, column], value)

    def build_tensor():
        for half in range(2):
            index = material_recv[:, half, :]
            for k in range(6):
                tensor[k, pl.ds(half * GZ, GZ), :] = entry(k, index)

    def apply_material(band):
        for at in range(0, N, 32):
            xx, yy, zz, xy, yz, zx = [tensor[k, pl.ds(at, 32), :] for k in range(6)]
            for part in range(2):
                for group in range(2):
                    rows, lanes = pl.ds(part * N + at, 32), pl.ds(group * N, N)
                    fx, fy, fz = [field[band * 3 + c, rows, lanes] for c in range(3)]
                    scaled[band * 3, rows, lanes] = xx * fx + xy * fy + zx * fz
                    scaled[band * 3 + 1, rows, lanes] = xy * fx + yy * fy + yz * fz
                    scaled[band * 3 + 2, rows, lanes] = zx * fx + yz * fy + zz * fz

    chunk_of_others(recv1, recv_sem.at[0]).wait()
    inverse_z(0, 1)
    spread(2, send1, recv1, 0)
    pltpu.make_async_copy(
        material_recv.at[pl.ds(0, GZ - 1)], material_recv.at[pl.ds(0, GZ - 1)], recv_sem.at[6]
    ).wait()
    build_tensor()
    chunk_of_others(recv1, recv_sem.at[1]).wait()
    inverse_z(2, 3)
    apply_material(0)
    forward_z(0, 1)
    spread(0, send2, recv2, 3)
    chunk_of_others(recv1, recv_sem.at[2]).wait()
    inverse_z(4, 5)
    apply_material(1)
    forward_z(2, 3)
    spread(1, send2, recv2, 3)
    forward_z(4, 5)
    spread(2, send2, recv2, 3)

    def gram_step(i, sums):
        sums = list(sums)
        for c in range(3):
            values = []
            for ref in (field, scaled):
                values.append(
                    [
                        [
                            ref[(e % 2) * 3 + c, pl.ds(pl.multiple_of(part * N + i * 8, 8), 8), pl.ds((e // 2) * N, N)]
                            for part in range(2)
                        ]
                        for e in range(4)
                    ]
                )
            f, s = values
            for a in range(4):
                for e in range(4):
                    k = a * 4 + e
                    sums[k] = sums[k] + (f[a][0] * s[e][0] + f[a][1] * s[e][1])
                    sums[16 + k] = sums[16 + k] + (f[a][0] * s[e][1] - f[a][1] * s[e][0])
        return tuple(sums)

    sums = lax.fori_loop(0, N // 8, gram_step, tuple(jnp.zeros((8, N), jnp.float32) for _ in range(32)))
    lane = lax.broadcasted_iota(jnp.int32, (1, N), 1)
    packed = jnp.zeros((1, N), jnp.float32)
    for k in range(32):
        total = jnp.sum(jnp.sum(sums[k], axis=0, keepdims=True), axis=1, keepdims=True)
        packed = packed + jnp.where(lane == k, total, 0.0)
    gram_send[0] = packed
    gram_recv[mine] = packed

    def gram_to(to, row):
        pltpu.make_async_remote_copy(
            src_ref=gram_send.at[0],
            dst_ref=gram_recv.at[mine],
            send_sem=send_sem.at[7],
            recv_sem=recv_sem.at[7],
            device_id=to,
            device_id_type=LOGICAL,
        ).start()

    to_known(gram_to)
    to_rest(gram_to)

    def forward_yx(*qs):
        columns = []
        for q in qs:
            halves = []
            for part in range(2):
                halves.append(
                    jnp.concatenate(
                        [
                            recv2[q // 2, pl.ds((q % 2) * 4 + part * 2 + plane, N, stride=8), :]
                            for plane in range(2)
                        ],
                        axis=1,
                    )
                )
            columns.append(jnp.concatenate(halves, axis=0))
        out = table_times(table, 0, jnp.concatenate(columns, axis=1))
        blocks = [swap_blocks(out[:, i * 2 * N : (i + 1) * 2 * N]) for i in range(len(qs))]
        rows = times_table(jnp.concatenate(blocks, axis=0), table, 1)
        for i, q in enumerate(qs):
            work[q] = rows[i * 2 * N : (i + 1) * 2 * N]

    chunk_of_others(recv2, recv_sem.at[3]).wait()
    forward_yx(0, 1)
    chunk_of_others(recv2, recv_sem.at[4]).wait()
    forward_yx(2, 3)
    chunk_of_others(recv2, recv_sem.at[5]).wait()
    forward_yx(4, 5)

    pltpu.make_async_copy(gram_recv.at[pl.ds(0, DEV - 1)], gram_recv.at[pl.ds(0, DEV - 1)], recv_sem.at[7]).wait()
    sums_ref[...] = jnp.sum(gram_recv[...], axis=0) * (1.0 / (N * N * N))

    for chunk in range(CHUNKS):
        chunk_of_others(send1, send_sem.at[chunk]).wait()
        chunk_of_others(send2, send_sem.at[3 + chunk]).wait()
    pltpu.make_async_copy(
        material_send.at[pl.ds(0, GZ - 1)], material_send.at[pl.ds(0, GZ - 1)], send_sem.at[6]
    ).wait()
    pltpu.make_async_copy(gram_recv.at[pl.ds(0, DEV - 1)], gram_recv.at[pl.ds(0, DEV - 1)], send_sem.at[7]).wait()


def curl_kernel(work, sums_ref, theta_hbm, gram_ref, theta, out_sem):
    qx, qy, qz = wavevectors(lax.axis_index("gz"))
    stores = []
    for band in range(2):
        for plane in range(2):
            for part in range(2):
                rows, lanes = block(plane, part)
                bx, by, bz = [work[band * 3 + c, rows, lanes] for c in range(3)]
                theta[band, part, 0, plane] = qz[plane] * by - qy * bz
                theta[band, part, 1, plane] = qx * bz - qz[plane] * bx
                theta[band, part, 2, plane] = qy * bx - qx * by
        stores.append(pltpu.make_async_copy(theta.at[band], theta_hbm.at[:, :, band], out_sem.at[band]))
        stores[-1].start()
    first = lax.axis_index("ba") * 2
    lane = lax.broadcasted_iota(jnp.int32, (4, N), 1)
    row = lax.broadcasted_iota(jnp.int32, (4, N), 0)
    start = lax.div(row, 2) * 16 + lax.rem(row, 2) + first
    whole = sums_ref[...]
    columns = [jnp.sum(jnp.where(lane == start + a * 4, whole, 0.0), axis=1, keepdims=True) for a in range(4)]
    gram = jnp.concatenate(columns, axis=1)
    gram_ref[0] = gram[:2]
    gram_ref[1] = gram[2:]
    for store in stores:
        store.wait()


def in_hbm(array):
    return pltpu.with_memory_space_constraint(array, pltpu.HBM)


def on_device(coeffs, material, inv_diag, inv_off):
    f32 = jnp.float32
    anywhere = pl.BlockSpec(memory_space=pltpu.HBM)
    smem = pl.BlockSpec(memory_space=pltpu.SMEM)
    vmem = pl.BlockSpec(memory_space=pltpu.VMEM)
    back, sums = pl.pallas_call(
        kernel,
        out_shape=(jax.ShapeDtypeStruct((6, 2 * N, 2 * N), f32), jax.ShapeDtypeStruct((1, N), f32)),
        in_specs=[anywhere, anywhere, smem, smem, anywhere],
        out_specs=(vmem, vmem),
        scratch_shapes=[
            pltpu.VMEM((2, 2, 3, 2, N, N), f32),
            pltpu.VMEM((2, N, N), jnp.int32),
            pltpu.VMEM((4, 2, 2 * N, 2 * N), jnp.bfloat16),
            pltpu.VMEM((CHUNKS, DEV * 8, N), f32),
            pltpu.VMEM((CHUNKS, DEV * 8, N), f32),
            pltpu.VMEM((6, 2 * N, 2 * N), f32),
            pltpu.VMEM((6, 2 * N, 2 * N), f32),
            pltpu.VMEM((CHUNKS, DEV * 8, N), f32),
            pltpu.VMEM((CHUNKS, DEV * 8, N), f32),
            pltpu.VMEM((DEV, 2, N), jnp.int32),
            pltpu.VMEM((GZ, 2, N), jnp.int32),
            pltpu.VMEM((6, N, N), f32),
            pltpu.VMEM((1, 1, N), f32),
            pltpu.VMEM((DEV, 1, N), f32),
            pltpu.SemaphoreType.DMA((4,)),
            pltpu.SemaphoreType.DMA((8,)),
            pltpu.SemaphoreType.DMA((8,)),
            pltpu.SemaphoreType.REGULAR,
        ],
        compiler_params=pltpu.CompilerParams(
            collective_id=0, has_side_effects=True, vmem_limit_bytes=32 * 1024 * 1024
        ),
        name="maxwell",
    )(in_hbm(coeffs), in_hbm(material), in_hbm(inv_diag), in_hbm(inv_off), in_hbm(jnp.asarray(tables())))
    theta, gram = pl.pallas_call(
        curl_kernel,
        out_shape=(jax.ShapeDtypeStruct(coeffs.shape, f32), jax.ShapeDtypeStruct((2, 2, 4), f32)),
        in_specs=[vmem, vmem],
        out_specs=(anywhere, vmem),
        scratch_shapes=[pltpu.VMEM((2, 2, 3, 2, N, N), f32), pltpu.SemaphoreType.DMA((2,))],
        compiler_params=pltpu.CompilerParams(vmem_limit_bytes=16 * 1024 * 1024),
        name="curl",
    )(back, sums)
    return theta, jnp.transpose(gram, (0, 2, 1))


def solution(mesh):
    in_specs = (P(None, None, "ba", "gz", None, None), P("gz", None, None), P(), P())
    out_specs = (P(None, None, "ba", "gz", None, None), P(None, None, "ba"))
    return jax.shard_map(
        on_device, mesh=mesh, in_specs=in_specs, out_specs=out_specs, check_vma=False
    )
```

```python
import jax
import jax.numpy as jnp
import numpy as np
from jax import lax
from jax.experimental import pallas as pl
from jax.experimental.pallas import tpu as pltpu
from jax.sharding import PartitionSpec as P

LOGICAL = pl.DeviceIdType.LOGICAL
N = 128
GZ = 64
DEV = 128
CHUNKS = 3
PLACES = ((0, 0), (0, 1), (1, 0), (1, 1), (3, 0), (3, 1), (2, 0), (2, 1))
SEEN_FROM = (0, 1, 4, 5, 2, 3, 6, 7)


def reverse_bits_np(values, levels):
    flipped = np.zeros_like(values)
    for position in range(levels):
        flipped = flipped + ((values >> position) & 1) * (1 << (levels - 1 - position))
    return flipped


def as_parts(table):
    high = table.astype(jnp.bfloat16)
    low = (table - high.astype(np.float64)).astype(jnp.bfloat16)
    return np.stack([high, low])


def tables():
    index = np.arange(N)
    scale = 1.0 / np.sqrt(N)
    angle = 2.0 * np.pi / N * (index[:, None] * index[None, :] % N)
    cosine, sine = np.cos(angle) * scale, np.sin(angle) * scale
    first = np.block([[cosine, sine], [-sine, cosine]])
    second = np.block([[cosine, -sine], [sine, cosine]])
    device = np.arange(GZ)
    planes = np.concatenate([device * 2, device * 2 + 1])
    reversed_device = reverse_bits_np(device, 6)
    numbers = np.concatenate([reversed_device, reversed_device + GZ])
    angle = 2.0 * np.pi / N * (planes[:, None] * numbers[None, :] % N)
    cosine, sine = np.cos(angle) * scale, np.sin(angle) * scale
    inverse = np.block([[cosine, -sine], [sine, cosine]])
    return np.stack([as_parts(t) for t in (first, second, inverse, inverse.T)])


def split(values):
    high = values.astype(jnp.bfloat16)
    low = (values - high.astype(jnp.float32)).astype(jnp.bfloat16)
    return high, low


def dot(left, right):
    return jnp.dot(left, right, preferred_element_type=jnp.float32)


def times_table(data, table_ref, which):
    high, low = split(data)
    return dot(high, table_ref[which, 0]) + (dot(low, table_ref[which, 0]) + dot(high, table_ref[which, 1]))


def table_times(table_ref, which, data):
    high, low = split(data)
    return dot(table_ref[which, 0], high) + (dot(table_ref[which, 0], low) + dot(table_ref[which, 1], high))


def swap_blocks(values):
    top = jnp.concatenate([values[:N, :N], values[N:, :N]], axis=1)
    bottom = jnp.concatenate([values[:N, N:], values[N:, N:]], axis=1)
    return jnp.concatenate([top, bottom], axis=0)


def wavevectors(gz):
    qx = lax.broadcasted_iota(jnp.int32, (N, N), 1)
    qx = jnp.where(qx < N // 2, qx, qx - N).astype(jnp.float32) * (1.0 / (N // 2))
    qy = lax.broadcasted_iota(jnp.int32, (N, N), 0)
    qy = jnp.where(qy < N // 2, qy, qy - N).astype(jnp.float32) * (1.0 / (N // 2))
    flipped = 0
    rest = gz
    for _ in range(6):
        flipped = flipped * 2 + lax.rem(rest, 2)
        rest = lax.div(rest, 2)
    qz = [flipped.astype(jnp.float32) * (1.0 / (N // 2)), (flipped - N // 2).astype(jnp.float32) * (1.0 / (N // 2))]
    return qx, qy, qz


def block(plane, part):
    return pl.ds(plane * N, N), pl.ds(part * N, N)


def kernel(
    coeffs_hbm, material_hbm, diag_ref, off_ref, tables_hbm,
    work, sums_ref,
    coeffs, material, table, send1, recv1, field, scaled, send2, recv2,
    material_send, material_recv, tensor, gram_send, gram_line, gram_lines,
    in_sem, send_sem, recv_sem, group_sem,
):
    gz = lax.axis_index("gz")
    ba = lax.axis_index("ba")
    me = gz * 2 + ba
    mine = ba * GZ + gz

    line, place = lax.div(me, 8), lax.rem(me, 8)
    core, across = lax.rem(gz, 2), ba * 2 + lax.rem(lax.div(gz, 2), 2)
    barrier = pltpu.get_barrier_semaphore()
    places = []
    for shift, other in PLACES:
        x = lax.rem(across + shift, 4)
        places.append(lax.rem(x, 2) * 4 + lax.rem(core + other, 2) * 2 + lax.div(x, 2))
    rows_of = [lax.rem(p, 2) * GZ + lax.div(p, 2) for p in places]

    def line_at(i):
        return lax.rem(line + i, 16)

    for i in range(1, 16):
        pl.semaphore_signal(barrier, inc=1, device_id=line_at(i) * 8 + place, device_id_type=LOGICAL)
    for i in range(1, 8):
        pl.semaphore_signal(barrier, inc=1, device_id=line * 8 + places[i], device_id_type=LOGICAL)

    loads = [
        pltpu.make_async_copy(coeffs_hbm.at[:, :, band], coeffs.at[band], in_sem.at[band]) for band in range(2)
    ]
    table_load = pltpu.make_async_copy(tables_hbm, table, in_sem.at[2])
    material_load = pltpu.make_async_copy(material_hbm, material, in_sem.at[3])
    loads[0].start()
    table_load.start()
    loads[1].start()
    material_load.start()

    qx, qy, qz = wavevectors(gz)

    def to_place(send, *which):
        def one(i, carry):
            there = line_at(i)
            for k in which:
                send(there * 8 + places[k], there * 4 + rows_of[k])
            return carry

        lax.fori_loop(1, 16, one, 0, unroll=5 if len(which) == 1 else 1)

    def to_line(send, *which):
        for k in which:
            send(line * 8 + places[k], line * 4 + rows_of[k])

    def to_all(send):
        to_place(send, *range(8))
        to_line(send, *range(1, 8))

    def piece(chunk, source, target, base, arrival=None):
        def send(to, row):
            pltpu.make_async_remote_copy(
                src_ref=source.at[chunk, pl.ds(pl.multiple_of(row * 8, 8), 8)],
                dst_ref=target.at[chunk, pl.ds(pl.multiple_of(mine * 8, 8), 8)],
                send_sem=send_sem.at[base + chunk],
                recv_sem=recv_sem.at[base + chunk if arrival is None else arrival],
                device_id=to,
                device_id_type=LOGICAL,
            ).start()

        return send

    def keep(chunk, source, target):
        own = pl.ds(pl.multiple_of(mine * 8, 8), 8)
        target[chunk, own, :] = source[chunk, own, :]

    def spread(chunk, source, target, base):
        send = piece(chunk, source, target, base)
        to_all(send)
        keep(chunk, source, target)

    def chunk_of_others(ref, sem, count=DEV - 1):
        rows = count * 8
        return pltpu.make_async_copy(ref.at[0, pl.ds(0, rows)], ref.at[0, pl.ds(0, rows)], sem)

    def forward_xy(*qs):
        rows = times_table(jnp.concatenate([work[q] for q in qs], axis=0), table, 0)
        blocks = [swap_blocks(rows[i * 2 * N : (i + 1) * 2 * N]) for i in range(len(qs))]
        out = table_times(table, 1, jnp.concatenate(blocks, axis=1))
        for i, q in enumerate(qs):
            for part in range(2):
                for plane in range(2):
                    row = (q % 2) * 4 + part * 2 + plane
                    start = i * 2 * N + plane * N
                    send1[q // 2, pl.ds(row, N, stride=8), :] = out[part * N : (part + 1) * N, start : start + N]

    def curl_in(band):
        for plane in range(2):
            for part in range(2):
                hx, hy, hz = [coeffs[band, part, c, plane] for c in range(3)]
                rows, lanes = block(plane, part)
                work[band * 3, rows, lanes] = qy * hz - qz[plane] * hy
                work[band * 3 + 1, rows, lanes] = qz[plane] * hx - qx * hz
                work[band * 3 + 2, rows, lanes] = qx * hy - qy * hx

    loads[0].wait()
    curl_in(0)
    table_load.wait()
    forward_xy(0, 1)
    material_load.wait()
    for plane in range(2):
        material_send[:, plane, :] = material[plane]

    def material_to(to, row):
        pltpu.make_async_remote_copy(
            src_ref=material_send.at[row],
            dst_ref=material_recv.at[gz],
            send_sem=send_sem.at[6],
            recv_sem=recv_sem.at[6],
            device_id=to,
            device_id_type=LOGICAL,
        ).start()

    def material_to_place(there):
        start = lax.rem(there, 2) * GZ + lax.div(there, 2)

        def one(i, carry):
            material_to(line_at(i) * 8 + there, line_at(i) * 4 + start)
            return carry

        lax.fori_loop(1, 16, one, 0, unroll=5)

    def material_to_line(there):
        to = line * 8 + there
        material_to(to, lax.rem(to, 2) * GZ + lax.div(to, 2))

    first = piece(0, send1, recv1, 0)
    pl.semaphore_wait(barrier, 22)
    for k in range(1, 8):
        pl.semaphore_signal(
            group_sem.at[SEEN_FROM[k]], inc=1, device_id=line * 8 + places[k], device_id_type=LOGICAL
        )
    material_to_place(place)
    to_place(first, 0)
    to_line(first, *range(1, 8))
    pl.semaphore_wait(group_sem.at[1], 1)
    to_place(first, 1)
    for k in range(2, 4):
        pl.semaphore_wait(group_sem.at[k], 1)
    to_place(first, 2, 3)
    for k in range(4, 6):
        pl.semaphore_wait(group_sem.at[k], 1)
    to_place(first, 4, 5)
    aside = lax.rem(place + 4, 8)
    for there in (places[1], aside, aside + places[1] - place):
        material_to_line(there)
        material_to_place(there)
    for k in range(6, 8):
        pl.semaphore_wait(group_sem.at[k], 1)
    to_place(first, 6, 7)
    keep(0, send1, recv1)
    material_recv[gz] = material_send[mine]
    loads[1].wait()
    curl_in(1)
    forward_xy(2, 3)
    spread(1, send1, recv1, 0)
    forward_xy(4, 5)

    def inverse_z(*qs):
        columns = []
        for q in qs:
            lines = []
            for part in range(2):
                for plane in range(2):
                    row = (q % 2) * 4 + part * 2 + plane
                    lines.append(
                        jnp.concatenate(
                            [recv1[q // 2, pl.ds(group * GZ * 8 + row, GZ, stride=8), :] for group in range(2)],
                            axis=1,
                        )
                    )
            columns.append(jnp.concatenate(lines, axis=0))
        out = table_times(table, 2, jnp.concatenate(columns, axis=1))
        for i, q in enumerate(qs):
            field[q] = out[:, i * 2 * N : (i + 1) * 2 * N]

    def forward_z(*qs):
        out = table_times(table, 3, jnp.concatenate([scaled[q] for q in qs], axis=1))
        for i, q in enumerate(qs):
            for part in range(2):
                for plane in range(2):
                    row = (q % 2) * 4 + part * 2 + plane
                    start = (part * 2 + plane) * GZ
                    for group in range(2):
                        lanes = i * 2 * N + group * N
                        send2[q // 2, pl.ds(group * GZ * 8 + row, GZ, stride=8), :] = out[
                            start : start + GZ, lanes : lanes + N
                        ]

    def entry(k, index):
        ref, column = (diag_ref, k) if k < 3 else (off_ref, k - 3)
        value = jnp.where(index == 1, ref[1, column], ref[0, column])
        value = jnp.where(index == 2, ref[2, column], value)
        return jnp.where(index == 3, ref[3, column], value)

    def build_tensor():
        for half in range(2):
            index = material_recv[:, half, :]
            for k in range(6):
                tensor[k, pl.ds(half * GZ, GZ), :] = entry(k, index)

    def apply_material(band):
        for at in range(0, N, 32):
            xx, yy, zz, xy, yz, zx = [tensor[k, pl.ds(at, 32), :] for k in range(6)]
            for part in range(2):
                for group in range(2):
                    rows, lanes = pl.ds(part * N + at, 32), pl.ds(group * N, N)
                    fx, fy, fz = [field[band * 3 + c, rows, lanes] for c in range(3)]
                    scaled[band * 3, rows, lanes] = xx * fx + xy * fy + zx * fz
                    scaled[band * 3 + 1, rows, lanes] = xy * fx + yy * fy + yz * fz
                    scaled[band * 3 + 2, rows, lanes] = zx * fx + yz * fy + zz * fz

    chunk_of_others(recv1, recv_sem.at[0]).wait()
    inverse_z(0, 1)
    spread(2, send1, recv1, 0)
    pltpu.make_async_copy(
        material_recv.at[pl.ds(0, GZ - 1)], material_recv.at[pl.ds(0, GZ - 1)], recv_sem.at[6]
    ).wait()
    build_tensor()
    chunk_of_others(recv1, recv_sem.at[1]).wait()
    inverse_z(2, 3)
    apply_material(0)
    forward_z(0, 1)
    spread(0, send2, recv2, 3)
    chunk_of_others(recv1, recv_sem.at[2]).wait()
    inverse_z(4, 5)
    apply_material(1)

    forward_z(2, 3)
    spread(1, send2, recv2, 3)

    def gram_step(i, sums):
        sums = list(sums)
        for c in range(3):
            values = []
            for ref in (field, scaled):
                values.append(
                    [
                        [
                            ref[(e % 2) * 3 + c, pl.ds(pl.multiple_of(part * N + i * 8, 8), 8), pl.ds((e // 2) * N, N)]
                            for part in range(2)
                        ]
                        for e in range(4)
                    ]
                )
            f, s = values
            for a in range(4):
                for e in range(4):
                    k = a * 4 + e
                    sums[k] = sums[k] + (f[a][0] * s[e][0] + f[a][1] * s[e][1])
                    sums[16 + k] = sums[16 + k] + (f[a][0] * s[e][1] - f[a][1] * s[e][0])
        return tuple(sums)

    sums = lax.fori_loop(0, N // 8, gram_step, tuple(jnp.zeros((8, N), jnp.float32) for _ in range(32)))
    lane = lax.broadcasted_iota(jnp.int32, (1, N), 1)
    packed = jnp.zeros((1, N), jnp.float32)
    for k in range(32):
        total = jnp.sum(jnp.sum(sums[k], axis=0, keepdims=True), axis=1, keepdims=True)
        packed = packed + jnp.where(lane == k, total, 0.0)
    gram_send[0] = packed
    gram_line[place] = packed

    def gram_to(slots, slot, sem):
        def send(to, row):
            pltpu.make_async_remote_copy(
                src_ref=gram_send.at[sem],
                dst_ref=slots.at[slot],
                send_sem=send_sem.at[7 + sem],
                recv_sem=recv_sem.at[7 + sem],
                device_id=to,
                device_id_type=LOGICAL,
            ).start()

        return send

    def gram_wait(slots, count, sem):
        pltpu.make_async_copy(slots.at[pl.ds(0, count)], slots.at[pl.ds(0, count)], sem).wait()

    to_line(gram_to(gram_line, place, 0), *range(1, 8))

    forward_z(4, 5)
    spread(2, send2, recv2, 3)

    def forward_yx(*qs):
        columns = []
        for q in qs:
            halves = []
            for part in range(2):
                halves.append(
                    jnp.concatenate(
                        [
                            recv2[q // 2, pl.ds((q % 2) * 4 + part * 2 + plane, N, stride=8), :]
                            for plane in range(2)
                        ],
                        axis=1,
                    )
                )
            columns.append(jnp.concatenate(halves, axis=0))
        out = table_times(table, 0, jnp.concatenate(columns, axis=1))
        blocks = [swap_blocks(out[:, i * 2 * N : (i + 1) * 2 * N]) for i in range(len(qs))]
        rows = times_table(jnp.concatenate(blocks, axis=0), table, 1)
        for i, q in enumerate(qs):
            work[q] = rows[i * 2 * N : (i + 1) * 2 * N]

    chunk_of_others(recv2, recv_sem.at[3]).wait()
    forward_yx(0, 1)
    gram_wait(gram_line, 7, recv_sem.at[7])
    line_sum = jnp.sum(gram_line[...], axis=0)
    gram_send[1] = line_sum
    gram_lines[line] = line_sum
    to_place(gram_to(gram_lines, line, 1), 0)
    chunk_of_others(recv2, recv_sem.at[4]).wait()
    forward_yx(2, 3)
    chunk_of_others(recv2, recv_sem.at[5]).wait()
    forward_yx(4, 5)

    gram_wait(gram_lines, 15, recv_sem.at[8])
    sums_ref[...] = jnp.sum(gram_lines[...], axis=0) * (1.0 / (N * N * N))

    for chunk in range(CHUNKS):
        chunk_of_others(send1, send_sem.at[chunk]).wait()
        chunk_of_others(send2, send_sem.at[3 + chunk]).wait()
    pltpu.make_async_copy(
        material_send.at[pl.ds(0, GZ - 1)], material_send.at[pl.ds(0, GZ - 1)], send_sem.at[6]
    ).wait()
    gram_wait(gram_line, 7, send_sem.at[7])
    gram_wait(gram_lines, 15, send_sem.at[8])


def curl_kernel(work, sums_ref, theta_hbm, gram_ref, theta, out_sem):
    qx, qy, qz = wavevectors(lax.axis_index("gz"))
    stores = []
    for band in range(2):
        for plane in range(2):
            for part in range(2):
                rows, lanes = block(plane, part)
                bx, by, bz = [work[band * 3 + c, rows, lanes] for c in range(3)]
                theta[band, part, 0, plane] = qz[plane] * by - qy * bz
                theta[band, part, 1, plane] = qx * bz - qz[plane] * bx
                theta[band, part, 2, plane] = qy * bx - qx * by
        stores.append(pltpu.make_async_copy(theta.at[band], theta_hbm.at[:, :, band], out_sem.at[band]))
        stores[-1].start()
    first = lax.axis_index("ba") * 2
    lane = lax.broadcasted_iota(jnp.int32, (4, N), 1)
    row = lax.broadcasted_iota(jnp.int32, (4, N), 0)
    start = lax.div(row, 2) * 16 + lax.rem(row, 2) + first
    whole = sums_ref[...]
    columns = [jnp.sum(jnp.where(lane == start + a * 4, whole, 0.0), axis=1, keepdims=True) for a in range(4)]
    gram = jnp.concatenate(columns, axis=1)
    gram_ref[0] = gram[:2]
    gram_ref[1] = gram[2:]
    for store in stores:
        store.wait()


def in_hbm(array):
    return pltpu.with_memory_space_constraint(array, pltpu.HBM)


def on_device(coeffs, material, inv_diag, inv_off):
    f32 = jnp.float32
    anywhere = pl.BlockSpec(memory_space=pltpu.HBM)
    smem = pl.BlockSpec(memory_space=pltpu.SMEM)
    vmem = pl.BlockSpec(memory_space=pltpu.VMEM)
    back, sums = pl.pallas_call(
        kernel,
        out_shape=(jax.ShapeDtypeStruct((6, 2 * N, 2 * N), f32), jax.ShapeDtypeStruct((1, N), f32)),
        in_specs=[anywhere, anywhere, smem, smem, anywhere],
        out_specs=(vmem, vmem),
        scratch_shapes=[
            pltpu.VMEM((2, 2, 3, 2, N, N), f32),
            pltpu.VMEM((2, N, N), jnp.int32),
            pltpu.VMEM((4, 2, 2 * N, 2 * N), jnp.bfloat16),
            pltpu.VMEM((CHUNKS, DEV * 8, N), f32),
            pltpu.VMEM((CHUNKS, DEV * 8, N), f32),
            pltpu.VMEM((6, 2 * N, 2 * N), f32),
            pltpu.VMEM((6, 2 * N, 2 * N), f32),
            pltpu.VMEM((CHUNKS, DEV * 8, N), f32),
            pltpu.VMEM((CHUNKS, DEV * 8, N), f32),
            pltpu.VMEM((DEV, 2, N), jnp.int32),
            pltpu.VMEM((GZ, 2, N), jnp.int32),
            pltpu.VMEM((6, N, N), f32),
            pltpu.VMEM((2, 1, N), f32),
            pltpu.VMEM((8, 1, N), f32),
            pltpu.VMEM((16, 1, N), f32),
            pltpu.SemaphoreType.DMA((4,)),
            pltpu.SemaphoreType.DMA((9,)),
            pltpu.SemaphoreType.DMA((10,)),
            pltpu.SemaphoreType.REGULAR((8,)),
        ],
        compiler_params=pltpu.CompilerParams(
            collective_id=0, has_side_effects=True, vmem_limit_bytes=32 * 1024 * 1024
        ),
        name="maxwell",
    )(in_hbm(coeffs), in_hbm(material), in_hbm(inv_diag), in_hbm(inv_off), in_hbm(jnp.asarray(tables())))
    theta, gram = pl.pallas_call(
        curl_kernel,
        out_shape=(jax.ShapeDtypeStruct(coeffs.shape, f32), jax.ShapeDtypeStruct((2, 2, 4), f32)),
        in_specs=[vmem, vmem],
        out_specs=(anywhere, vmem),
        scratch_shapes=[pltpu.VMEM((2, 2, 3, 2, N, N), f32), pltpu.SemaphoreType.DMA((2,))],
        compiler_params=pltpu.CompilerParams(vmem_limit_bytes=16 * 1024 * 1024),
        name="curl",
    )(back, sums)
    return theta, jnp.transpose(gram, (0, 2, 1))


def solution(mesh):
    in_specs = (P(None, None, "ba", "gz", None, None), P("gz", None, None), P(), P())
    out_specs = (P(None, None, "ba", "gz", None, None), P(None, None, "ba"))
    return jax.shard_map(
        on_device, mesh=mesh, in_specs=in_specs, out_specs=out_specs, check_vma=False
    )
```

```python
import jax
import jax.numpy as jnp
import numpy as np
from jax import lax
from jax.experimental import pallas as pl
from jax.experimental.pallas import tpu as pltpu
from jax.sharding import PartitionSpec as P

LOGICAL = pl.DeviceIdType.LOGICAL
N = 128
GZ = 64
DEV = 128
CHUNKS = 3
PLACES = ((0, 0), (0, 1), (1, 0), (1, 1), (3, 0), (3, 1), (2, 0), (2, 1))
SEEN_FROM = (0, 1, 4, 5, 2, 3, 6, 7)


def reverse_bits_np(values, levels):
    flipped = np.zeros_like(values)
    for position in range(levels):
        flipped = flipped + ((values >> position) & 1) * (1 << (levels - 1 - position))
    return flipped


def as_parts(table):
    high = table.astype(jnp.bfloat16)
    low = (table - high.astype(np.float64)).astype(jnp.bfloat16)
    return np.stack([high, low])


def tables():
    index = np.arange(N)
    scale = 1.0 / np.sqrt(N)
    angle = 2.0 * np.pi / N * (index[:, None] * index[None, :] % N)
    cosine, sine = np.cos(angle) * scale, np.sin(angle) * scale
    first = np.block([[cosine, sine], [-sine, cosine]])
    second = np.block([[cosine, -sine], [sine, cosine]])
    device = np.arange(GZ)
    planes = np.concatenate([device * 2, device * 2 + 1])
    reversed_device = reverse_bits_np(device, 6)
    numbers = np.concatenate([reversed_device, reversed_device + GZ])
    angle = 2.0 * np.pi / N * (planes[:, None] * numbers[None, :] % N)
    cosine, sine = np.cos(angle) * scale, np.sin(angle) * scale
    inverse = np.block([[cosine, -sine], [sine, cosine]])
    return np.stack([as_parts(t) for t in (first, second, inverse, inverse.T)])


def split(values):
    high = values.astype(jnp.bfloat16)
    low = (values - high.astype(jnp.float32)).astype(jnp.bfloat16)
    return high, low


def dot(left, right):
    return jnp.dot(left, right, preferred_element_type=jnp.float32)


def times_table(data, table_ref, which):
    high, low = split(data)
    return dot(high, table_ref[which, 0]) + (dot(low, table_ref[which, 0]) + dot(high, table_ref[which, 1]))


def table_times(table_ref, which, data):
    high, low = split(data)
    return dot(table_ref[which, 0], high) + (dot(table_ref[which, 0], low) + dot(table_ref[which, 1], high))


def swap_blocks(values):
    top = jnp.concatenate([values[:N, :N], values[N:, :N]], axis=1)
    bottom = jnp.concatenate([values[:N, N:], values[N:, N:]], axis=1)
    return jnp.concatenate([top, bottom], axis=0)


def wavevectors(gz):
    qx = lax.broadcasted_iota(jnp.int32, (N, N), 1)
    qx = jnp.where(qx < N // 2, qx, qx - N).astype(jnp.float32) * (1.0 / (N // 2))
    qy = lax.broadcasted_iota(jnp.int32, (N, N), 0)
    qy = jnp.where(qy < N // 2, qy, qy - N).astype(jnp.float32) * (1.0 / (N // 2))
    flipped = 0
    rest = gz
    for _ in range(6):
        flipped = flipped * 2 + lax.rem(rest, 2)
        rest = lax.div(rest, 2)
    qz = [flipped.astype(jnp.float32) * (1.0 / (N // 2)), (flipped - N // 2).astype(jnp.float32) * (1.0 / (N // 2))]
    return qx, qy, qz


def block(plane, part):
    return pl.ds(plane * N, N), pl.ds(part * N, N)


def kernel(
    coeffs_hbm, material_hbm, diag_hbm, off_hbm, tables_hbm,
    work, sums_ref,
    coeffs, material, diag_ref, off_ref, table, send1, recv1, field, scaled, send2, recv2,
    material_send, material_recv, tensor, gram_send, gram_line, gram_lines,
    in_sem, send_sem, recv_sem, group_sem,
):
    gz = lax.axis_index("gz")
    ba = lax.axis_index("ba")
    me = gz * 2 + ba
    mine = ba * GZ + gz

    line, place = lax.div(me, 8), lax.rem(me, 8)
    core, across = lax.rem(gz, 2), ba * 2 + lax.rem(lax.div(gz, 2), 2)
    barrier = pltpu.get_barrier_semaphore()

    def line_at(i):
        return lax.rem(line + i, 16)

    for i in range(1, 16):
        pl.semaphore_signal(barrier, inc=1, device_id=line_at(i) * 8 + place, device_id_type=LOGICAL)
    places = []
    for shift, other in PLACES:
        x = lax.rem(across + shift, 4)
        places.append(lax.rem(x, 2) * 4 + lax.rem(core + other, 2) * 2 + lax.div(x, 2))
    rows_of = [lax.rem(p, 2) * GZ + lax.div(p, 2) for p in places]

    for i in range(1, 8):
        pl.semaphore_signal(barrier, inc=1, device_id=line * 8 + places[i], device_id_type=LOGICAL)

    loads = [
        pltpu.make_async_copy(coeffs_hbm.at[:, :, band], coeffs.at[band], in_sem.at[band]) for band in range(2)
    ]
    table_load = pltpu.make_async_copy(tables_hbm, table, in_sem.at[2])
    material_load = pltpu.make_async_copy(material_hbm, material, in_sem.at[3])
    loads[0].start()
    table_load.start()
    loads[1].start()
    material_load.start()
    diag_load = pltpu.make_async_copy(diag_hbm, diag_ref, in_sem.at[4])
    off_load = pltpu.make_async_copy(off_hbm, off_ref, in_sem.at[5])
    diag_load.start()
    off_load.start()

    qx, qy, qz = wavevectors(gz)

    def to_place(send, *which):
        def one(i, carry):
            there = line_at(i)
            for k in which:
                send(there * 8 + places[k], there * 4 + rows_of[k])
            return carry

        lax.fori_loop(1, 16, one, 0, unroll=5 if len(which) == 1 else 1)

    def to_line(send, *which):
        for k in which:
            send(line * 8 + places[k], line * 4 + rows_of[k])

    def to_all(send):
        to_place(send, *range(8))
        to_line(send, *range(1, 8))

    def piece(chunk, source, target, base, arrival=None):
        def send(to, row):
            pltpu.make_async_remote_copy(
                src_ref=source.at[chunk, pl.ds(pl.multiple_of(row * 8, 8), 8)],
                dst_ref=target.at[chunk, pl.ds(pl.multiple_of(mine * 8, 8), 8)],
                send_sem=send_sem.at[base + chunk],
                recv_sem=recv_sem.at[base + chunk if arrival is None else arrival],
                device_id=to,
                device_id_type=LOGICAL,
            ).start()

        return send

    def keep(chunk, source, target):
        own = pl.ds(pl.multiple_of(mine * 8, 8), 8)
        target[chunk, own, :] = source[chunk, own, :]

    def spread(chunk, source, target, base):
        send = piece(chunk, source, target, base)
        to_all(send)
        keep(chunk, source, target)

    def chunk_of_others(ref, sem, count=DEV - 1):
        rows = count * 8
        return pltpu.make_async_copy(ref.at[0, pl.ds(0, rows)], ref.at[0, pl.ds(0, rows)], sem)

    def forward_xy(*qs):
        rows = times_table(jnp.concatenate([work[q] for q in qs], axis=0), table, 0)
        blocks = [swap_blocks(rows[i * 2 * N : (i + 1) * 2 * N]) for i in range(len(qs))]
        out = table_times(table, 1, jnp.concatenate(blocks, axis=1))
        for i, q in enumerate(qs):
            for part in range(2):
                for plane in range(2):
                    row = (q % 2) * 4 + part * 2 + plane
                    start = i * 2 * N + plane * N
                    send1[q // 2, pl.ds(row, N, stride=8), :] = out[part * N : (part + 1) * N, start : start + N]

    def curl_in(band):
        for plane in range(2):
            for part in range(2):
                hx, hy, hz = [coeffs[band, part, c, plane] for c in range(3)]
                rows, lanes = block(plane, part)
                work[band * 3, rows, lanes] = qy * hz - qz[plane] * hy
                work[band * 3 + 1, rows, lanes] = qz[plane] * hx - qx * hz
                work[band * 3 + 2, rows, lanes] = qx * hy - qy * hx

    loads[0].wait()
    curl_in(0)
    table_load.wait()
    forward_xy(0, 1)
    material_load.wait()
    for plane in range(2):
        material_send[:, plane, :] = material[plane]

    def material_to(to, row):
        pltpu.make_async_remote_copy(
            src_ref=material_send.at[row],
            dst_ref=material_recv.at[gz],
            send_sem=send_sem.at[6],
            recv_sem=recv_sem.at[6],
            device_id=to,
            device_id_type=LOGICAL,
        ).start()

    def material_to_place(there):
        start = lax.rem(there, 2) * GZ + lax.div(there, 2)

        def one(i, carry):
            material_to(line_at(i) * 8 + there, line_at(i) * 4 + start)
            return carry

        lax.fori_loop(1, 16, one, 0, unroll=5)

    def material_to_line(there):
        to = line * 8 + there
        material_to(to, lax.rem(to, 2) * GZ + lax.div(to, 2))

    first = piece(0, send1, recv1, 0)
    pl.semaphore_wait(barrier, 22)
    for k in range(1, 8):
        pl.semaphore_signal(
            group_sem.at[SEEN_FROM[k]], inc=1, device_id=line * 8 + places[k], device_id_type=LOGICAL
        )
    material_to_place(place)
    to_place(first, 0)
    to_line(first, *range(1, 8))
    pl.semaphore_wait(group_sem.at[1], 1)
    to_place(first, 1)
    for k in range(2, 4):
        pl.semaphore_wait(group_sem.at[k], 1)
    to_place(first, 2, 3)
    for k in range(4, 6):
        pl.semaphore_wait(group_sem.at[k], 1)
    to_place(first, 4, 5)
    aside = lax.rem(place + 4, 8)
    for there in (places[1], aside, aside + places[1] - place):
        material_to_line(there)
        material_to_place(there)
    for k in range(6, 8):
        pl.semaphore_wait(group_sem.at[k], 1)
    to_place(first, 6, 7)
    keep(0, send1, recv1)
    material_recv[gz] = material_send[mine]
    loads[1].wait()
    curl_in(1)
    forward_xy(2, 3)
    spread(1, send1, recv1, 0)
    forward_xy(4, 5)

    def inverse_z(*qs):
        columns = []
        for q in qs:
            lines = []
            for part in range(2):
                for plane in range(2):
                    row = (q % 2) * 4 + part * 2 + plane
                    lines.append(
                        jnp.concatenate(
                            [recv1[q // 2, pl.ds(group * GZ * 8 + row, GZ, stride=8), :] for group in range(2)],
                            axis=1,
                        )
                    )
            columns.append(jnp.concatenate(lines, axis=0))
        out = table_times(table, 2, jnp.concatenate(columns, axis=1))
        for i, q in enumerate(qs):
            field[q] = out[:, i * 2 * N : (i + 1) * 2 * N]

    def forward_z(*qs):
        out = table_times(table, 3, jnp.concatenate([scaled[q] for q in qs], axis=1))
        for i, q in enumerate(qs):
            for part in range(2):
                for plane in range(2):
                    row = (q % 2) * 4 + part * 2 + plane
                    start = (part * 2 + plane) * GZ
                    for group in range(2):
                        lanes = i * 2 * N + group * N
                        send2[q // 2, pl.ds(group * GZ * 8 + row, GZ, stride=8), :] = out[
                            start : start + GZ, lanes : lanes + N
                        ]

    def entry(k, index):
        ref, column = (diag_ref, k) if k < 3 else (off_ref, k - 3)
        value = jnp.where(index == 1, ref[1, column], ref[0, column])
        value = jnp.where(index == 2, ref[2, column], value)
        return jnp.where(index == 3, ref[3, column], value)

    def build_tensor():
        for half in range(2):
            index = material_recv[:, half, :]
            for k in range(6):
                tensor[k, pl.ds(half * GZ, GZ), :] = entry(k, index)

    def apply_material(band):
        for at in range(0, N, 32):
            xx, yy, zz, xy, yz, zx = [tensor[k, pl.ds(at, 32), :] for k in range(6)]
            for part in range(2):
                for group in range(2):
                    rows, lanes = pl.ds(part * N + at, 32), pl.ds(group * N, N)
                    fx, fy, fz = [field[band * 3 + c, rows, lanes] for c in range(3)]
                    scaled[band * 3, rows, lanes] = xx * fx + xy * fy + zx * fz
                    scaled[band * 3 + 1, rows, lanes] = xy * fx + yy * fy + yz * fz
                    scaled[band * 3 + 2, rows, lanes] = zx * fx + yz * fy + zz * fz

    chunk_of_others(recv1, recv_sem.at[0]).wait()
    inverse_z(0, 1)
    spread(2, send1, recv1, 0)
    pltpu.make_async_copy(
        material_recv.at[pl.ds(0, GZ - 1)], material_recv.at[pl.ds(0, GZ - 1)], recv_sem.at[6]
    ).wait()
    diag_load.wait()
    off_load.wait()
    build_tensor()
    chunk_of_others(recv1, recv_sem.at[1]).wait()
    inverse_z(2, 3)
    apply_material(0)
    forward_z(0, 1)
    spread(0, send2, recv2, 3)
    chunk_of_others(recv1, recv_sem.at[2]).wait()
    inverse_z(4, 5)
    apply_material(1)

    forward_z(2, 3)
    spread(1, send2, recv2, 3)

    def gram_step(i, sums):
        sums = list(sums)
        for c in range(3):
            values = []
            for ref in (field, scaled):
                values.append(
                    [
                        [
                            ref[(e % 2) * 3 + c, pl.ds(pl.multiple_of(part * N + i * 8, 8), 8), pl.ds((e // 2) * N, N)]
                            for part in range(2)
                        ]
                        for e in range(4)
                    ]
                )
            f, s = values
            for a in range(4):
                for e in range(4):
                    k = a * 4 + e
                    sums[k] = sums[k] + (f[a][0] * s[e][0] + f[a][1] * s[e][1])
                    sums[16 + k] = sums[16 + k] + (f[a][0] * s[e][1] - f[a][1] * s[e][0])
        return tuple(sums)

    sums = lax.fori_loop(0, N // 8, gram_step, tuple(jnp.zeros((8, N), jnp.float32) for _ in range(32)))
    lane = lax.broadcasted_iota(jnp.int32, (1, N), 1)
    packed = jnp.zeros((1, N), jnp.float32)
    for k in range(32):
        total = jnp.sum(jnp.sum(sums[k], axis=0, keepdims=True), axis=1, keepdims=True)
        packed = packed + jnp.where(lane == k, total, 0.0)
    gram_send[0] = packed
    gram_line[place] = packed

    def gram_to(slots, slot, sem):
        def send(to, row):
            pltpu.make_async_remote_copy(
                src_ref=gram_send.at[sem],
                dst_ref=slots.at[slot],
                send_sem=send_sem.at[7 + sem],
                recv_sem=recv_sem.at[7 + sem],
                device_id=to,
                device_id_type=LOGICAL,
            ).start()

        return send

    def gram_wait(slots, count, sem):
        pltpu.make_async_copy(slots.at[pl.ds(0, count)], slots.at[pl.ds(0, count)], sem).wait()

    to_line(gram_to(gram_line, place, 0), *range(1, 8))

    forward_z(4, 5)
    spread(2, send2, recv2, 3)

    def forward_yx(*qs):
        columns = []
        for q in qs:
            halves = []
            for part in range(2):
                halves.append(
                    jnp.concatenate(
                        [
                            recv2[q // 2, pl.ds((q % 2) * 4 + part * 2 + plane, N, stride=8), :]
                            for plane in range(2)
                        ],
                        axis=1,
                    )
                )
            columns.append(jnp.concatenate(halves, axis=0))
        out = table_times(table, 0, jnp.concatenate(columns, axis=1))
        blocks = [swap_blocks(out[:, i * 2 * N : (i + 1) * 2 * N]) for i in range(len(qs))]
        rows = times_table(jnp.concatenate(blocks, axis=0), table, 1)
        for i, q in enumerate(qs):
            work[q] = rows[i * 2 * N : (i + 1) * 2 * N]

    chunk_of_others(recv2, recv_sem.at[3]).wait()
    forward_yx(0, 1)
    gram_wait(gram_line, 7, recv_sem.at[7])
    line_sum = jnp.sum(gram_line[...], axis=0)
    gram_send[1] = line_sum
    gram_lines[line] = line_sum
    to_place(gram_to(gram_lines, line, 1), 0)
    chunk_of_others(recv2, recv_sem.at[4]).wait()
    forward_yx(2, 3)
    chunk_of_others(recv2, recv_sem.at[5]).wait()
    forward_yx(4, 5)

    gram_wait(gram_lines, 15, recv_sem.at[8])
    sums_ref[...] = jnp.sum(gram_lines[...], axis=0) * (1.0 / (N * N * N))

    for chunk in range(CHUNKS):
        chunk_of_others(send1, send_sem.at[chunk]).wait()
        chunk_of_others(send2, send_sem.at[3 + chunk]).wait()
    pltpu.make_async_copy(
        material_send.at[pl.ds(0, GZ - 1)], material_send.at[pl.ds(0, GZ - 1)], send_sem.at[6]
    ).wait()
    gram_wait(gram_line, 7, send_sem.at[7])
    gram_wait(gram_lines, 15, send_sem.at[8])


def curl_kernel(work, sums_ref, theta_hbm, gram_ref, theta, out_sem):
    qx, qy, qz = wavevectors(lax.axis_index("gz"))
    stores = []
    for band in range(2):
        for part in range(2):
            for plane in range(2):
                rows, lanes = block(plane, part)
                bx, by, bz = [work[band * 3 + c, rows, lanes] for c in range(3)]
                theta[band, part, 0, plane] = qz[plane] * by - qy * bz
                theta[band, part, 1, plane] = qx * bz - qz[plane] * bx
                theta[band, part, 2, plane] = qy * bx - qx * by
            store = pltpu.make_async_copy(
                theta.at[band, part], theta_hbm.at[part, :, band], out_sem.at[band * 2 + part]
            )
            store.start()
            stores.append(store)
    first = lax.axis_index("ba") * 2
    lane = lax.broadcasted_iota(jnp.int32, (4, N), 1)
    row = lax.broadcasted_iota(jnp.int32, (4, N), 0)
    start = lax.div(row, 2) * 16 + lax.rem(row, 2) + first
    whole = sums_ref[...]
    columns = [jnp.sum(jnp.where(lane == start + a * 4, whole, 0.0), axis=1, keepdims=True) for a in range(4)]
    gram = jnp.concatenate(columns, axis=1)
    gram_ref[0] = gram[:2]
    gram_ref[1] = gram[2:]
    for store in stores:
        store.wait()


def in_hbm(array):
    return pltpu.with_memory_space_constraint(array, pltpu.HBM)


def on_device(coeffs, material, inv_diag, inv_off):
    f32 = jnp.float32
    anywhere = pl.BlockSpec(memory_space=pltpu.HBM)
    vmem = pl.BlockSpec(memory_space=pltpu.VMEM)
    back, sums = pl.pallas_call(
        kernel,
        out_shape=(jax.ShapeDtypeStruct((6, 2 * N, 2 * N), f32), jax.ShapeDtypeStruct((1, N), f32)),
        in_specs=[anywhere] * 5,
        out_specs=(vmem, vmem),
        scratch_shapes=[
            pltpu.VMEM((2, 2, 3, 2, N, N), f32),
            pltpu.VMEM((2, N, N), jnp.int32),
            pltpu.SMEM((4, 3), f32),
            pltpu.SMEM((4, 3), f32),
            pltpu.VMEM((4, 2, 2 * N, 2 * N), jnp.bfloat16),
            pltpu.VMEM((CHUNKS, DEV * 8, N), f32),
            pltpu.VMEM((CHUNKS, DEV * 8, N), f32),
            pltpu.VMEM((6, 2 * N, 2 * N), f32),
            pltpu.VMEM((6, 2 * N, 2 * N), f32),
            pltpu.VMEM((CHUNKS, DEV * 8, N), f32),
            pltpu.VMEM((CHUNKS, DEV * 8, N), f32),
            pltpu.VMEM((DEV, 2, N), jnp.int32),
            pltpu.VMEM((GZ, 2, N), jnp.int32),
            pltpu.VMEM((6, N, N), f32),
            pltpu.VMEM((2, 1, N), f32),
            pltpu.VMEM((8, 1, N), f32),
            pltpu.VMEM((16, 1, N), f32),
            pltpu.SemaphoreType.DMA((6,)),
            pltpu.SemaphoreType.DMA((9,)),
            pltpu.SemaphoreType.DMA((10,)),
            pltpu.SemaphoreType.REGULAR((8,)),
        ],
        compiler_params=pltpu.CompilerParams(
            collective_id=0, has_side_effects=True, vmem_limit_bytes=32 * 1024 * 1024
        ),
        name="maxwell",
    )(in_hbm(coeffs), in_hbm(material), in_hbm(inv_diag), in_hbm(inv_off), in_hbm(jnp.asarray(tables())))
    theta, gram = pl.pallas_call(
        curl_kernel,
        out_shape=(jax.ShapeDtypeStruct(coeffs.shape, f32), jax.ShapeDtypeStruct((2, 2, 4), f32)),
        in_specs=[vmem, vmem],
        out_specs=(anywhere, vmem),
        scratch_shapes=[pltpu.VMEM((2, 2, 3, 2, N, N), f32), pltpu.SemaphoreType.DMA((4,))],
        compiler_params=pltpu.CompilerParams(vmem_limit_bytes=16 * 1024 * 1024),
        name="curl",
    )(back, sums)
    return theta, jnp.transpose(gram, (0, 2, 1))


def solution(mesh):
    in_specs = (P(None, None, "ba", "gz", None, None), P("gz", None, None), P(), P())
    out_specs = (P(None, None, "ba", "gz", None, None), P(None, None, "ba"))
    return jax.shard_map(
        on_device, mesh=mesh, in_specs=in_specs, out_specs=out_specs, check_vma=False
    )
```

```python
import jax
import jax.numpy as jnp
import numpy as np
from jax import lax
from jax.experimental import pallas as pl
from jax.experimental.pallas import tpu as pltpu
from jax.sharding import PartitionSpec as P

LOGICAL = pl.DeviceIdType.LOGICAL
N = 128
GZ = 64
DEV = 128
CHUNKS = 3
PLACES = ((0, 0), (0, 1), (1, 0), (1, 1), (3, 0), (3, 1), (2, 0), (2, 1))
SEEN_FROM = (0, 1, 4, 5, 2, 3, 6, 7)


def reverse_bits_np(values, levels):
    flipped = np.zeros_like(values)
    for position in range(levels):
        flipped = flipped + ((values >> position) & 1) * (1 << (levels - 1 - position))
    return flipped


def as_parts(table):
    high = table.astype(jnp.bfloat16)
    low = (table - high.astype(np.float64)).astype(jnp.bfloat16)
    return np.stack([high, low])


def tables():
    index = np.arange(N)
    scale = 1.0 / np.sqrt(N)
    angle = 2.0 * np.pi / N * (index[:, None] * index[None, :] % N)
    cosine, sine = np.cos(angle) * scale, np.sin(angle) * scale
    first = np.block([[cosine, sine], [-sine, cosine]])
    second = np.block([[cosine, -sine], [sine, cosine]])
    device = np.arange(GZ)
    planes = np.concatenate([device * 2, device * 2 + 1])
    reversed_device = reverse_bits_np(device, 6)
    numbers = np.concatenate([reversed_device, reversed_device + GZ])
    angle = 2.0 * np.pi / N * (planes[:, None] * numbers[None, :] % N)
    cosine, sine = np.cos(angle) * scale, np.sin(angle) * scale
    inverse = np.block([[cosine, -sine], [sine, cosine]])
    return np.stack([as_parts(t) for t in (first, second, inverse, inverse.T)])


def split(values):
    high = values.astype(jnp.bfloat16)
    low = (values - high.astype(jnp.float32)).astype(jnp.bfloat16)
    return high, low


def dot(left, right):
    return jnp.dot(left, right, preferred_element_type=jnp.float32)


def times_table(data, table_ref, which):
    high, low = split(data)
    return dot(high, table_ref[which, 0]) + (dot(low, table_ref[which, 0]) + dot(high, table_ref[which, 1]))


def table_times(table_ref, which, data):
    high, low = split(data)
    return dot(table_ref[which, 0], high) + (dot(table_ref[which, 0], low) + dot(table_ref[which, 1], high))


def swap_blocks(values):
    top = jnp.concatenate([values[:N, :N], values[N:, :N]], axis=1)
    bottom = jnp.concatenate([values[:N, N:], values[N:, N:]], axis=1)
    return jnp.concatenate([top, bottom], axis=0)


def wavevectors(gz):
    qx = lax.broadcasted_iota(jnp.int32, (N, N), 1)
    qx = jnp.where(qx < N // 2, qx, qx - N).astype(jnp.float32) * (1.0 / (N // 2))
    qy = lax.broadcasted_iota(jnp.int32, (N, N), 0)
    qy = jnp.where(qy < N // 2, qy, qy - N).astype(jnp.float32) * (1.0 / (N // 2))
    flipped = 0
    rest = gz
    for _ in range(6):
        flipped = flipped * 2 + lax.rem(rest, 2)
        rest = lax.div(rest, 2)
    qz = [flipped.astype(jnp.float32) * (1.0 / (N // 2)), (flipped - N // 2).astype(jnp.float32) * (1.0 / (N // 2))]
    return qx, qy, qz


def block(plane, part):
    return pl.ds(plane * N, N), pl.ds(part * N, N)


def kernel(
    coeffs_hbm, material_hbm, diag_hbm, off_hbm, tables_hbm,
    work, sums_ref,
    coeffs, material, diag_ref, off_ref, table, send1, recv1, field, scaled, send2, recv2,
    material_send, material_recv, tensor, gram_send, gram_line, gram_lines,
    in_sem, send_sem, recv_sem, group_sem,
):
    gz = lax.axis_index("gz")
    ba = lax.axis_index("ba")
    me = gz * 2 + ba
    mine = ba * GZ + gz

    line, place = lax.div(me, 8), lax.rem(me, 8)
    core, across = lax.rem(gz, 2), ba * 2 + lax.rem(lax.div(gz, 2), 2)
    barrier = pltpu.get_barrier_semaphore()

    def line_at(i):
        return lax.rem(line + i, 16)

    z, y = lax.div(line, 4), lax.rem(line, 4)
    for dz, dy in ((2, 2), (2, 1), (2, 3), (1, 2), (3, 2), (2, 0), (0, 2), (1, 1), (1, 3), (3, 1), (3, 3), (1, 0), (3, 0), (0, 1), (0, 3)):
        there = lax.rem(z + dz, 4) * 4 + lax.rem(y + dy, 4)
        pl.semaphore_signal(barrier, inc=1, device_id=there * 8 + place, device_id_type=LOGICAL)
    places = []
    for shift, other in PLACES:
        x = lax.rem(across + shift, 4)
        places.append(lax.rem(x, 2) * 4 + lax.rem(core + other, 2) * 2 + lax.div(x, 2))
    rows_of = [lax.rem(p, 2) * GZ + lax.div(p, 2) for p in places]

    for i in range(1, 8):
        pl.semaphore_signal(barrier, inc=1, device_id=line * 8 + places[i], device_id_type=LOGICAL)

    loads = [
        pltpu.make_async_copy(coeffs_hbm.at[:, :, band], coeffs.at[band], in_sem.at[band]) for band in range(2)
    ]
    table_load = pltpu.make_async_copy(tables_hbm, table, in_sem.at[2])
    material_load = pltpu.make_async_copy(material_hbm, material, in_sem.at[3])
    loads[0].start()
    table_load.start()
    loads[1].start()
    material_load.start()
    diag_load = pltpu.make_async_copy(diag_hbm, diag_ref, in_sem.at[4])
    off_load = pltpu.make_async_copy(off_hbm, off_ref, in_sem.at[5])
    diag_load.start()
    off_load.start()

    qx, qy, qz = wavevectors(gz)

    def to_place(send, *which):
        def one(i, carry):
            there = line_at(i)
            for k in which:
                send(there * 8 + places[k], there * 4 + rows_of[k])
            return carry

        lax.fori_loop(1, 16, one, 0, unroll=5 if len(which) == 1 else 1)

    def to_line(send, *which):
        for k in which:
            send(line * 8 + places[k], line * 4 + rows_of[k])

    def to_all(send):
        to_place(send, *range(8))
        to_line(send, *range(1, 8))

    def piece(chunk, source, target, base, arrival=None):
        def send(to, row):
            pltpu.make_async_remote_copy(
                src_ref=source.at[chunk, pl.ds(pl.multiple_of(row * 8, 8), 8)],
                dst_ref=target.at[chunk, pl.ds(pl.multiple_of(mine * 8, 8), 8)],
                send_sem=send_sem.at[base + chunk],
                recv_sem=recv_sem.at[base + chunk if arrival is None else arrival],
                device_id=to,
                device_id_type=LOGICAL,
            ).start()

        return send

    def keep(chunk, source, target):
        own = pl.ds(pl.multiple_of(mine * 8, 8), 8)
        target[chunk, own, :] = source[chunk, own, :]

    def spread(chunk, source, target, base):
        send = piece(chunk, source, target, base)
        to_all(send)
        keep(chunk, source, target)

    def chunk_of_others(ref, sem, count=DEV - 1):
        rows = count * 8
        return pltpu.make_async_copy(ref.at[0, pl.ds(0, rows)], ref.at[0, pl.ds(0, rows)], sem)

    def forward_xy(*qs):
        rows = times_table(jnp.concatenate([work[q] for q in qs], axis=0), table, 0)
        blocks = [swap_blocks(rows[i * 2 * N : (i + 1) * 2 * N]) for i in range(len(qs))]
        out = table_times(table, 1, jnp.concatenate(blocks, axis=1))
        for i, q in enumerate(qs):
            for part in range(2):
                for plane in range(2):
                    row = (q % 2) * 4 + part * 2 + plane
                    start = i * 2 * N + plane * N
                    send1[q // 2, pl.ds(row, N, stride=8), :] = out[part * N : (part + 1) * N, start : start + N]

    def curl_in(band):
        for plane in range(2):
            for part in range(2):
                hx, hy, hz = [coeffs[band, part, c, plane] for c in range(3)]
                rows, lanes = block(plane, part)
                work[band * 3, rows, lanes] = qy * hz - qz[plane] * hy
                work[band * 3 + 1, rows, lanes] = qz[plane] * hx - qx * hz
                work[band * 3 + 2, rows, lanes] = qx * hy - qy * hx

    loads[0].wait()
    curl_in(0)
    table_load.wait()
    forward_xy(0, 1)
    material_load.wait()
    for plane in range(2):
        material_send[:, plane, :] = material[plane]

    def material_to(to, row):
        pltpu.make_async_remote_copy(
            src_ref=material_send.at[row],
            dst_ref=material_recv.at[gz],
            send_sem=send_sem.at[6],
            recv_sem=recv_sem.at[6],
            device_id=to,
            device_id_type=LOGICAL,
        ).start()

    def material_to_place(there):
        start = lax.rem(there, 2) * GZ + lax.div(there, 2)

        def one(i, carry):
            material_to(line_at(i) * 8 + there, line_at(i) * 4 + start)
            return carry

        lax.fori_loop(1, 16, one, 0, unroll=5)

    def material_to_line(there):
        to = line * 8 + there
        material_to(to, lax.rem(to, 2) * GZ + lax.div(to, 2))

    first = piece(0, send1, recv1, 0)
    last = piece(0, send1, recv1, 0, 9)
    pl.semaphore_wait(barrier, 22)
    for k in (2, 3, 4, 5, 6, 7, 1):
        pl.semaphore_signal(
            group_sem.at[SEEN_FROM[k]], inc=1, device_id=line * 8 + places[k], device_id_type=LOGICAL
        )
    material_to_place(place)
    to_place(first, 0)
    to_line(first, *range(1, 8))
    pl.semaphore_wait(group_sem.at[1], 1)
    to_place(first, 1)
    for k in range(2, 4):
        pl.semaphore_wait(group_sem.at[k], 1)
    to_place(first, 2, 3)
    for k in range(4, 6):
        pl.semaphore_wait(group_sem.at[k], 1)
    to_place(first, 4, 5)
    aside = lax.rem(place + 4, 8)
    for there in (places[1], aside, aside + places[1] - place):
        material_to_line(there)
        material_to_place(there)
    for k in range(6, 8):
        pl.semaphore_wait(group_sem.at[k], 1)
    to_place(last, 6, 7)
    keep(0, send1, recv1)
    material_recv[gz] = material_send[mine]
    loads[1].wait()
    curl_in(1)
    forward_xy(2, 3)
    spread(1, send1, recv1, 0)
    forward_xy(4, 5)

    def inverse_z(*qs):
        columns = []
        for q in qs:
            lines = []
            for part in range(2):
                for plane in range(2):
                    row = (q % 2) * 4 + part * 2 + plane
                    lines.append(
                        jnp.concatenate(
                            [recv1[q // 2, pl.ds(group * GZ * 8 + row, GZ, stride=8), :] for group in range(2)],
                            axis=1,
                        )
                    )
            columns.append(jnp.concatenate(lines, axis=0))
        out = table_times(table, 2, jnp.concatenate(columns, axis=1))
        for i, q in enumerate(qs):
            field[q] = out[:, i * 2 * N : (i + 1) * 2 * N]

    def forward_z(*qs):
        out = table_times(table, 3, jnp.concatenate([scaled[q] for q in qs], axis=1))
        for i, q in enumerate(qs):
            for part in range(2):
                for plane in range(2):
                    row = (q % 2) * 4 + part * 2 + plane
                    start = (part * 2 + plane) * GZ
                    for group in range(2):
                        lanes = i * 2 * N + group * N
                        send2[q // 2, pl.ds(group * GZ * 8 + row, GZ, stride=8), :] = out[
                            start : start + GZ, lanes : lanes + N
                        ]

    def entry(k, index):
        ref, column = (diag_ref, k) if k < 3 else (off_ref, k - 3)
        value = jnp.where(index == 1, ref[1, column], ref[0, column])
        value = jnp.where(index == 2, ref[2, column], value)
        return jnp.where(index == 3, ref[3, column], value)

    def build_tensor():
        for half in range(2):
            index = material_recv[:, half, :]
            for k in range(6):
                tensor[k, pl.ds(half * GZ, GZ), :] = entry(k, index)

    def apply_material(band):
        for at in range(0, N, 32):
            xx, yy, zz, xy, yz, zx = [tensor[k, pl.ds(at, 32), :] for k in range(6)]
            for part in range(2):
                for group in range(2):
                    rows, lanes = pl.ds(part * N + at, 32), pl.ds(group * N, N)
                    fx, fy, fz = [field[band * 3 + c, rows, lanes] for c in range(3)]
                    scaled[band * 3, rows, lanes] = xx * fx + xy * fy + zx * fz
                    scaled[band * 3 + 1, rows, lanes] = xy * fx + yy * fy + yz * fz
                    scaled[band * 3 + 2, rows, lanes] = zx * fx + yz * fy + zz * fz

    chunk_of_others(recv1, recv_sem.at[0], 97).wait()
    third = piece(2, send1, recv1, 0)
    to_place(third, 4, 5, 6, 7)
    chunk_of_others(recv1, recv_sem.at[9], 30).wait()
    inverse_z(0, 1)
    to_place(third, 0, 1, 2, 3)
    to_line(third, *range(1, 8))
    keep(2, send1, recv1)
    pltpu.make_async_copy(
        material_recv.at[pl.ds(0, GZ - 1)], material_recv.at[pl.ds(0, GZ - 1)], recv_sem.at[6]
    ).wait()
    diag_load.wait()
    off_load.wait()
    build_tensor()
    chunk_of_others(recv1, recv_sem.at[1]).wait()
    inverse_z(2, 3)
    apply_material(0)
    forward_z(0, 1)
    spread(0, send2, recv2, 3)
    chunk_of_others(recv1, recv_sem.at[2]).wait()
    inverse_z(4, 5)
    apply_material(1)

    forward_z(2, 3)
    spread(1, send2, recv2, 3)

    def gram_step(i, sums):
        sums = list(sums)
        for c in range(3):
            values = []
            for ref in (field, scaled):
                values.append(
                    [
                        [
                            ref[(e % 2) * 3 + c, pl.ds(pl.multiple_of(part * N + i * 8, 8), 8), pl.ds((e // 2) * N, N)]
                            for part in range(2)
                        ]
                        for e in range(4)
                    ]
                )
            f, s = values
            for a in range(4):
                for e in range(4):
                    k = a * 4 + e
                    sums[k] = sums[k] + (f[a][0] * s[e][0] + f[a][1] * s[e][1])
                    sums[16 + k] = sums[16 + k] + (f[a][0] * s[e][1] - f[a][1] * s[e][0])
        return tuple(sums)

    sums = lax.fori_loop(0, N // 8, gram_step, tuple(jnp.zeros((8, N), jnp.float32) for _ in range(32)))
    lane = lax.broadcasted_iota(jnp.int32, (1, N), 1)
    packed = jnp.zeros((1, N), jnp.float32)
    for k in range(32):
        total = jnp.sum(jnp.sum(sums[k], axis=0, keepdims=True), axis=1, keepdims=True)
        packed = packed + jnp.where(lane == k, total, 0.0)
    gram_send[0] = packed
    gram_line[place] = packed

    def gram_to(slots, slot, sem):
        def send(to, row):
            pltpu.make_async_remote_copy(
                src_ref=gram_send.at[sem],
                dst_ref=slots.at[slot],
                send_sem=send_sem.at[7 + sem],
                recv_sem=recv_sem.at[7 + sem],
                device_id=to,
                device_id_type=LOGICAL,
            ).start()

        return send

    def gram_wait(slots, count, sem):
        pltpu.make_async_copy(slots.at[pl.ds(0, count)], slots.at[pl.ds(0, count)], sem).wait()

    to_line(gram_to(gram_line, place, 0), *range(1, 8))

    forward_z(4, 5)
    spread(2, send2, recv2, 3)

    def forward_yx(*qs):
        columns = []
        for q in qs:
            halves = []
            for part in range(2):
                halves.append(
                    jnp.concatenate(
                        [
                            recv2[q // 2, pl.ds((q % 2) * 4 + part * 2 + plane, N, stride=8), :]
                            for plane in range(2)
                        ],
                        axis=1,
                    )
                )
            columns.append(jnp.concatenate(halves, axis=0))
        out = table_times(table, 0, jnp.concatenate(columns, axis=1))
        blocks = [swap_blocks(out[:, i * 2 * N : (i + 1) * 2 * N]) for i in range(len(qs))]
        rows = times_table(jnp.concatenate(blocks, axis=0), table, 1)
        for i, q in enumerate(qs):
            work[q] = rows[i * 2 * N : (i + 1) * 2 * N]

    chunk_of_others(recv2, recv_sem.at[3]).wait()
    forward_yx(0, 1)
    gram_wait(gram_line, 7, recv_sem.at[7])
    line_sum = jnp.sum(gram_line[...], axis=0)
    gram_send[1] = line_sum
    gram_lines[line] = line_sum
    to_place(gram_to(gram_lines, line, 1), 0)
    chunk_of_others(recv2, recv_sem.at[4]).wait()
    forward_yx(2, 3)
    chunk_of_others(recv2, recv_sem.at[5]).wait()
    forward_yx(4, 5)

    gram_wait(gram_lines, 15, recv_sem.at[8])
    sums_ref[...] = jnp.sum(gram_lines[...], axis=0) * (1.0 / (N * N * N))

    for chunk in range(CHUNKS):
        chunk_of_others(send1, send_sem.at[chunk]).wait()
        chunk_of_others(send2, send_sem.at[3 + chunk]).wait()
    pltpu.make_async_copy(
        material_send.at[pl.ds(0, GZ - 1)], material_send.at[pl.ds(0, GZ - 1)], send_sem.at[6]
    ).wait()
    gram_wait(gram_line, 7, send_sem.at[7])
    gram_wait(gram_lines, 15, send_sem.at[8])


def curl_kernel(work, sums_ref, theta_hbm, gram_ref, theta, out_sem):
    qx, qy, qz = wavevectors(lax.axis_index("gz"))
    stores = []
    for band in range(2):
        for part in range(2):
            for plane in range(2):
                rows, lanes = block(plane, part)
                bx, by, bz = [work[band * 3 + c, rows, lanes] for c in range(3)]
                theta[band, part, 0, plane] = qz[plane] * by - qy * bz
                theta[band, part, 1, plane] = qx * bz - qz[plane] * bx
                theta[band, part, 2, plane] = qy * bx - qx * by
            store = pltpu.make_async_copy(
                theta.at[band, part], theta_hbm.at[part, :, band], out_sem.at[band * 2 + part]
            )
            store.start()
            stores.append(store)
    first = lax.axis_index("ba") * 2
    lane = lax.broadcasted_iota(jnp.int32, (4, N), 1)
    row = lax.broadcasted_iota(jnp.int32, (4, N), 0)
    start = lax.div(row, 2) * 16 + lax.rem(row, 2) + first
    whole = sums_ref[...]
    columns = [jnp.sum(jnp.where(lane == start + a * 4, whole, 0.0), axis=1, keepdims=True) for a in range(4)]
    gram = jnp.concatenate(columns, axis=1)
    gram_ref[0] = gram[:2]
    gram_ref[1] = gram[2:]
    for store in stores:
        store.wait()


def in_hbm(array):
    return pltpu.with_memory_space_constraint(array, pltpu.HBM)


def on_device(coeffs, material, inv_diag, inv_off):
    f32 = jnp.float32
    anywhere = pl.BlockSpec(memory_space=pltpu.HBM)
    vmem = pl.BlockSpec(memory_space=pltpu.VMEM)
    back, sums = pl.pallas_call(
        kernel,
        out_shape=(jax.ShapeDtypeStruct((6, 2 * N, 2 * N), f32), jax.ShapeDtypeStruct((1, N), f32)),
        in_specs=[anywhere] * 5,
        out_specs=(vmem, vmem),
        scratch_shapes=[
            pltpu.VMEM((2, 2, 3, 2, N, N), f32),
            pltpu.VMEM((2, N, N), jnp.int32),
            pltpu.SMEM((4, 3), f32),
            pltpu.SMEM((4, 3), f32),
            pltpu.VMEM((4, 2, 2 * N, 2 * N), jnp.bfloat16),
            pltpu.VMEM((CHUNKS, DEV * 8, N), f32),
            pltpu.VMEM((CHUNKS, DEV * 8, N), f32),
            pltpu.VMEM((6, 2 * N, 2 * N), f32),
            pltpu.VMEM((6, 2 * N, 2 * N), f32),
            pltpu.VMEM((CHUNKS, DEV * 8, N), f32),
            pltpu.VMEM((CHUNKS, DEV * 8, N), f32),
            pltpu.VMEM((DEV, 2, N), jnp.int32),
            pltpu.VMEM((GZ, 2, N), jnp.int32),
            pltpu.VMEM((6, N, N), f32),
            pltpu.VMEM((2, 1, N), f32),
            pltpu.VMEM((8, 1, N), f32),
            pltpu.VMEM((16, 1, N), f32),
            pltpu.SemaphoreType.DMA((6,)),
            pltpu.SemaphoreType.DMA((9,)),
            pltpu.SemaphoreType.DMA((10,)),
            pltpu.SemaphoreType.REGULAR((8,)),
        ],
        compiler_params=pltpu.CompilerParams(
            collective_id=0, has_side_effects=True, vmem_limit_bytes=32 * 1024 * 1024
        ),
        name="maxwell",
    )(in_hbm(coeffs), in_hbm(material), in_hbm(inv_diag), in_hbm(inv_off), in_hbm(jnp.asarray(tables())))
    theta, gram = pl.pallas_call(
        curl_kernel,
        out_shape=(jax.ShapeDtypeStruct(coeffs.shape, f32), jax.ShapeDtypeStruct((2, 2, 4), f32)),
        in_specs=[vmem, vmem],
        out_specs=(anywhere, vmem),
        scratch_shapes=[pltpu.VMEM((2, 2, 3, 2, N, N), f32), pltpu.SemaphoreType.DMA((4,))],
        compiler_params=pltpu.CompilerParams(vmem_limit_bytes=16 * 1024 * 1024),
        name="curl",
    )(back, sums)
    return theta, jnp.transpose(gram, (0, 2, 1))


def solution(mesh):
    in_specs = (P(None, None, "ba", "gz", None, None), P("gz", None, None), P(), P())
    out_specs = (P(None, None, "ba", "gz", None, None), P(None, None, "ba"))
    return jax.shard_map(
        on_device, mesh=mesh, in_specs=in_specs, out_specs=out_specs, check_vma=False
    )
```

```python
import jax
import jax.numpy as jnp
import numpy as np
from jax import lax
from jax.experimental import pallas as pl
from jax.experimental.pallas import tpu as pltpu
from jax.sharding import PartitionSpec as P

LOGICAL = pl.DeviceIdType.LOGICAL
N = 128
GZ = 64
DEV = 128
CHUNKS = 3
PLACES = ((0, 0), (0, 1), (1, 0), (1, 1), (3, 0), (3, 1), (2, 0), (2, 1))
SEEN_FROM = (0, 1, 4, 5, 2, 3, 6, 7)


def reverse_bits_np(values, levels):
    flipped = np.zeros_like(values)
    for position in range(levels):
        flipped = flipped + ((values >> position) & 1) * (1 << (levels - 1 - position))
    return flipped


def as_parts(table):
    high = table.astype(jnp.bfloat16)
    low = (table - high.astype(np.float64)).astype(jnp.bfloat16)
    return np.stack([high, low])


def tables():
    index = np.arange(N)
    scale = 1.0 / np.sqrt(N)
    angle = 2.0 * np.pi / N * (index[:, None] * index[None, :] % N)
    cosine, sine = np.cos(angle) * scale, np.sin(angle) * scale
    first = np.block([[cosine, sine], [-sine, cosine]])
    second = np.block([[cosine, -sine], [sine, cosine]])
    device = np.arange(GZ)
    planes = np.concatenate([device * 2, device * 2 + 1])
    reversed_device = reverse_bits_np(device, 6)
    numbers = np.concatenate([reversed_device, reversed_device + GZ])
    angle = 2.0 * np.pi / N * (planes[:, None] * numbers[None, :] % N)
    cosine, sine = np.cos(angle) * scale, np.sin(angle) * scale
    inverse = np.block([[cosine, -sine], [sine, cosine]])
    return np.stack([as_parts(t) for t in (first, second, inverse, inverse.T)])


def split(values):
    high = values.astype(jnp.bfloat16)
    low = (values - high.astype(jnp.float32)).astype(jnp.bfloat16)
    return high, low


def dot(left, right):
    return jnp.dot(left, right, preferred_element_type=jnp.float32)


def times_table(data, table_ref, which):
    high, low = split(data)
    return dot(high, table_ref[which, 0]) + (dot(low, table_ref[which, 0]) + dot(high, table_ref[which, 1]))


def table_times(table_ref, which, data):
    high, low = split(data)
    return dot(table_ref[which, 0], high) + (dot(table_ref[which, 0], low) + dot(table_ref[which, 1], high))


def swap_blocks(values):
    top = jnp.concatenate([values[:N, :N], values[N:, :N]], axis=1)
    bottom = jnp.concatenate([values[:N, N:], values[N:, N:]], axis=1)
    return jnp.concatenate([top, bottom], axis=0)


def wavevectors(gz):
    qx = lax.broadcasted_iota(jnp.int32, (N, N), 1)
    qx = jnp.where(qx < N // 2, qx, qx - N).astype(jnp.float32) * (1.0 / (N // 2))
    qy = lax.broadcasted_iota(jnp.int32, (N, N), 0)
    qy = jnp.where(qy < N // 2, qy, qy - N).astype(jnp.float32) * (1.0 / (N // 2))
    flipped = 0
    rest = gz
    for _ in range(6):
        flipped = flipped * 2 + lax.rem(rest, 2)
        rest = lax.div(rest, 2)
    qz = [flipped.astype(jnp.float32) * (1.0 / (N // 2)), (flipped - N // 2).astype(jnp.float32) * (1.0 / (N // 2))]
    return qx, qy, qz


def block(plane, part):
    return pl.ds(plane * N, N), pl.ds(part * N, N)


def kernel(
    coeffs_hbm, material_hbm, diag_hbm, off_hbm, tables_hbm,
    work, sums_ref,
    coeffs, material, diag_ref, off_ref, table, send1, recv1, field, scaled, send2, recv2,
    material_send, material_recv, tensor, gram_send, gram_line, gram_lines,
    in_sem, send_sem, recv_sem, group_sem,
):
    gz = lax.axis_index("gz")
    ba = lax.axis_index("ba")
    me = gz * 2 + ba
    mine = ba * GZ + gz

    line, place = lax.div(me, 8), lax.rem(me, 8)
    core, across = lax.rem(gz, 2), ba * 2 + lax.rem(lax.div(gz, 2), 2)
    barrier = pltpu.get_barrier_semaphore()

    def line_at(i):
        return lax.rem(line + i, 16)

    for i in range(1, 16):
        pl.semaphore_signal(barrier, inc=1, device_id=line_at(i) * 8 + place, device_id_type=LOGICAL)
    places = []
    for shift, other in PLACES:
        x = lax.rem(across + shift, 4)
        places.append(lax.rem(x, 2) * 4 + lax.rem(core + other, 2) * 2 + lax.div(x, 2))
    rows_of = [lax.rem(p, 2) * GZ + lax.div(p, 2) for p in places]

    for i in range(1, 8):
        pl.semaphore_signal(barrier, inc=1, device_id=line * 8 + places[i], device_id_type=LOGICAL)

    loads = [
        pltpu.make_async_copy(coeffs_hbm.at[:, :, band], coeffs.at[band], in_sem.at[band]) for band in range(2)
    ]
    table_load = pltpu.make_async_copy(tables_hbm, table, in_sem.at[2])
    material_load = pltpu.make_async_copy(material_hbm, material, in_sem.at[3])
    loads[0].start()
    table_load.start()
    loads[1].start()
    material_load.start()
    diag_load = pltpu.make_async_copy(diag_hbm, diag_ref, in_sem.at[4])
    off_load = pltpu.make_async_copy(off_hbm, off_ref, in_sem.at[5])
    diag_load.start()
    off_load.start()

    qx, qy, qz = wavevectors(gz)

    def to_place(send, *which):
        def one(i, carry):
            there = line_at(i)
            for k in which:
                send(there * 8 + places[k], there * 4 + rows_of[k])
            return carry

        lax.fori_loop(1, 16, one, 0, unroll=5 if len(which) == 1 else 1)

    def to_line(send, *which):
        for k in which:
            send(line * 8 + places[k], line * 4 + rows_of[k])

    def to_all(send):
        to_place(send, *range(8))
        to_line(send, *range(1, 8))

    def piece(chunk, source, target, base, arrival=None):
        def send(to, row):
            pltpu.make_async_remote_copy(
                src_ref=source.at[chunk, pl.ds(pl.multiple_of(row * 8, 8), 8)],
                dst_ref=target.at[chunk, pl.ds(pl.multiple_of(mine * 8, 8), 8)],
                send_sem=send_sem.at[base + chunk],
                recv_sem=recv_sem.at[base + chunk if arrival is None else arrival],
                device_id=to,
                device_id_type=LOGICAL,
            ).start()

        return send

    def keep(chunk, source, target):
        own = pl.ds(pl.multiple_of(mine * 8, 8), 8)
        target[chunk, own, :] = source[chunk, own, :]

    def spread(chunk, source, target, base):
        send = piece(chunk, source, target, base)
        to_all(send)
        keep(chunk, source, target)

    def chunk_of_others(ref, sem, count=DEV - 1):
        rows = count * 8
        return pltpu.make_async_copy(ref.at[0, pl.ds(0, rows)], ref.at[0, pl.ds(0, rows)], sem)

    def forward_xy(*qs):
        rows = times_table(jnp.concatenate([work[q] for q in qs], axis=0), table, 0)
        blocks = [swap_blocks(rows[i * 2 * N : (i + 1) * 2 * N]) for i in range(len(qs))]
        out = table_times(table, 1, jnp.concatenate(blocks, axis=1))
        for i, q in enumerate(qs):
            for part in range(2):
                for plane in range(2):
                    row = (q % 2) * 4 + part * 2 + plane
                    start = i * 2 * N + plane * N
                    send1[q // 2, pl.ds(row, N, stride=8), :] = out[part * N : (part + 1) * N, start : start + N]

    def curl_in(band):
        for plane in range(2):
            for part in range(2):
                hx, hy, hz = [coeffs[band, part, c, plane] for c in range(3)]
                rows, lanes = block(plane, part)
                work[band * 3, rows, lanes] = qy * hz - qz[plane] * hy
                work[band * 3 + 1, rows, lanes] = qz[plane] * hx - qx * hz
                work[band * 3 + 2, rows, lanes] = qx * hy - qy * hx

    loads[0].wait()
    curl_in(0)
    table_load.wait()
    forward_xy(0, 1)
    material_load.wait()
    for plane in range(2):
        material_send[:, plane, :] = material[plane]

    def material_to(to, row):
        pltpu.make_async_remote_copy(
            src_ref=material_send.at[row],
            dst_ref=material_recv.at[gz],
            send_sem=send_sem.at[6],
            recv_sem=recv_sem.at[6],
            device_id=to,
            device_id_type=LOGICAL,
        ).start()

    def material_to_place(there):
        start = lax.rem(there, 2) * GZ + lax.div(there, 2)

        def one(i, carry):
            material_to(line_at(i) * 8 + there, line_at(i) * 4 + start)
            return carry

        lax.fori_loop(1, 16, one, 0, unroll=5)

    def material_to_line(there):
        to = line * 8 + there
        material_to(to, lax.rem(to, 2) * GZ + lax.div(to, 2))

    first = piece(0, send1, recv1, 0)
    pl.semaphore_wait(barrier, 22)
    for k in range(1, 8):
        pl.semaphore_signal(
            group_sem.at[SEEN_FROM[k]], inc=1, device_id=line * 8 + places[k], device_id_type=LOGICAL
        )
    material_to_place(place)
    to_place(first, 0)
    to_line(first, *range(1, 8))
    pl.semaphore_wait(group_sem.at[1], 1)
    to_place(first, 1)
    for k in range(2, 4):
        pl.semaphore_wait(group_sem.at[k], 1)
    to_place(first, 2, 3)
    for k in range(4, 6):
        pl.semaphore_wait(group_sem.at[k], 1)
    to_place(first, 4, 5)
    aside = lax.rem(place + 4, 8)
    for there in (places[1], aside, aside + places[1] - place):
        material_to_line(there)
        material_to_place(there)
    for k in range(6, 8):
        pl.semaphore_wait(group_sem.at[k], 1)
    to_place(first, 6, 7)
    keep(0, send1, recv1)
    material_recv[gz] = material_send[mine]
    loads[1].wait()
    curl_in(1)
    forward_xy(2, 3)
    spread(1, send1, recv1, 0)
    forward_xy(4, 5)

    def inverse_z(*qs):
        columns = []
        for q in qs:
            lines = []
            for part in range(2):
                for plane in range(2):
                    row = (q % 2) * 4 + part * 2 + plane
                    lines.append(
                        jnp.concatenate(
                            [recv1[q // 2, pl.ds(group * GZ * 8 + row, GZ, stride=8), :] for group in range(2)],
                            axis=1,
                        )
                    )
            columns.append(jnp.concatenate(lines, axis=0))
        out = table_times(table, 2, jnp.concatenate(columns, axis=1))
        for i, q in enumerate(qs):
            field[q] = out[:, i * 2 * N : (i + 1) * 2 * N]

    def forward_z(*qs):
        out = table_times(table, 3, jnp.concatenate([scaled[q] for q in qs], axis=1))
        for i, q in enumerate(qs):
            for part in range(2):
                for plane in range(2):
                    row = (q % 2) * 4 + part * 2 + plane
                    start = (part * 2 + plane) * GZ
                    for group in range(2):
                        lanes = i * 2 * N + group * N
                        send2[q // 2, pl.ds(group * GZ * 8 + row, GZ, stride=8), :] = out[
                            start : start + GZ, lanes : lanes + N
                        ]

    def entry(k, index):
        ref, column = (diag_ref, k) if k < 3 else (off_ref, k - 3)
        value = jnp.where(index == 1, ref[1, column], ref[0, column])
        value = jnp.where(index == 2, ref[2, column], value)
        return jnp.where(index == 3, ref[3, column], value)

    def build_tensor():
        for half in range(2):
            index = material_recv[:, half, :]
            for k in range(6):
                tensor[k, pl.ds(half * GZ, GZ), :] = entry(k, index)

    def apply_material(band):
        for at in range(0, N, 32):
            xx, yy, zz, xy, yz, zx = [tensor[k, pl.ds(at, 32), :] for k in range(6)]
            for part in range(2):
                for group in range(2):
                    rows, lanes = pl.ds(part * N + at, 32), pl.ds(group * N, N)
                    fx, fy, fz = [field[band * 3 + c, rows, lanes] for c in range(3)]
                    scaled[band * 3, rows, lanes] = xx * fx + xy * fy + zx * fz
                    scaled[band * 3 + 1, rows, lanes] = xy * fx + yy * fy + yz * fz
                    scaled[band * 3 + 2, rows, lanes] = zx * fx + yz * fy + zz * fz

    chunk_of_others(recv1, recv_sem.at[0]).wait()
    inverse_z(0, 1)
    spread(2, send1, recv1, 0)
    pltpu.make_async_copy(
        material_recv.at[pl.ds(0, GZ - 1)], material_recv.at[pl.ds(0, GZ - 1)], recv_sem.at[6]
    ).wait()
    diag_load.wait()
    off_load.wait()
    build_tensor()
    chunk_of_others(recv1, recv_sem.at[1]).wait()
    inverse_z(2, 3)
    apply_material(0)
    forward_z(0, 1)
    spread(0, send2, recv2, 3)
    chunk_of_others(recv1, recv_sem.at[2]).wait()
    inverse_z(4, 5)
    apply_material(1)

    forward_z(2, 3)
    spread(1, send2, recv2, 3)

    def gram_step(i, sums):
        sums = list(sums)
        for c in range(3):
            values = []
            for ref in (field, scaled):
                values.append(
                    [
                        [
                            ref[(e % 2) * 3 + c, pl.ds(pl.multiple_of(part * N + i * 8, 8), 8), pl.ds((e // 2) * N, N)]
                            for part in range(2)
                        ]
                        for e in range(4)
                    ]
                )
            f, s = values
            for a in range(4):
                for e in range(4):
                    k = a * 4 + e
                    sums[k] = sums[k] + (f[a][0] * s[e][0] + f[a][1] * s[e][1])
                    sums[16 + k] = sums[16 + k] + (f[a][0] * s[e][1] - f[a][1] * s[e][0])
        return tuple(sums)

    sums = lax.fori_loop(0, N // 8, gram_step, tuple(jnp.zeros((8, N), jnp.float32) for _ in range(32)))
    lane = lax.broadcasted_iota(jnp.int32, (1, N), 1)
    packed = jnp.zeros((1, N), jnp.float32)
    for k in range(32):
        total = jnp.sum(jnp.sum(sums[k], axis=0, keepdims=True), axis=1, keepdims=True)
        packed = packed + jnp.where(lane == k, total, 0.0)
    gram_send[0] = packed
    gram_line[place] = packed

    def gram_to(slots, slot, sem):
        def send(to, row):
            pltpu.make_async_remote_copy(
                src_ref=gram_send.at[sem],
                dst_ref=slots.at[slot],
                send_sem=send_sem.at[7 + sem],
                recv_sem=recv_sem.at[7 + sem],
                device_id=to,
                device_id_type=LOGICAL,
            ).start()

        return send

    def gram_wait(slots, count, sem):
        pltpu.make_async_copy(slots.at[pl.ds(0, count)], slots.at[pl.ds(0, count)], sem).wait()

    to_line(gram_to(gram_line, place, 0), *range(1, 8))

    forward_z(4, 5)
    spread(2, send2, recv2, 3)

    def forward_yx(*qs):
        columns = []
        for q in qs:
            halves = []
            for part in range(2):
                halves.append(
                    jnp.concatenate(
                        [
                            recv2[q // 2, pl.ds((q % 2) * 4 + part * 2 + plane, N, stride=8), :]
                            for plane in range(2)
                        ],
                        axis=1,
                    )
                )
            columns.append(jnp.concatenate(halves, axis=0))
        out = table_times(table, 0, jnp.concatenate(columns, axis=1))
        blocks = [swap_blocks(out[:, i * 2 * N : (i + 1) * 2 * N]) for i in range(len(qs))]
        rows = times_table(jnp.concatenate(blocks, axis=0), table, 1)
        for i, q in enumerate(qs):
            work[q] = rows[i * 2 * N : (i + 1) * 2 * N]

    chunk_of_others(recv2, recv_sem.at[3]).wait()
    forward_yx(0, 1)
    gram_wait(gram_line, 7, recv_sem.at[7])
    line_sum = jnp.sum(gram_line[...], axis=0)
    gram_send[1] = line_sum
    gram_lines[line] = line_sum
    to_place(gram_to(gram_lines, line, 1), 0)
    chunk_of_others(recv2, recv_sem.at[4]).wait()
    forward_yx(2, 3)
    chunk_of_others(recv2, recv_sem.at[5]).wait()
    forward_yx(4)
    forward_yx(5)

    gram_wait(gram_lines, 15, recv_sem.at[8])
    sums_ref[...] = jnp.sum(gram_lines[...], axis=0) * (1.0 / (N * N * N))

    for chunk in range(CHUNKS):
        chunk_of_others(send1, send_sem.at[chunk]).wait()
        chunk_of_others(send2, send_sem.at[3 + chunk]).wait()
    pltpu.make_async_copy(
        material_send.at[pl.ds(0, GZ - 1)], material_send.at[pl.ds(0, GZ - 1)], send_sem.at[6]
    ).wait()
    gram_wait(gram_line, 7, send_sem.at[7])
    gram_wait(gram_lines, 15, send_sem.at[8])


def curl_kernel(work, sums_ref, theta_hbm, gram_ref, theta, out_sem):
    qx, qy, qz = wavevectors(lax.axis_index("gz"))
    stores = []
    for band in range(2):
        for part in range(2):
            for plane in range(2):
                rows, lanes = block(plane, part)
                bx, by, bz = [work[band * 3 + c, rows, lanes] for c in range(3)]
                theta[band, part, 0, plane] = qz[plane] * by - qy * bz
                theta[band, part, 1, plane] = qx * bz - qz[plane] * bx
                theta[band, part, 2, plane] = qy * bx - qx * by
            store = pltpu.make_async_copy(
                theta.at[band, part], theta_hbm.at[part, :, band], out_sem.at[band * 2 + part]
            )
            store.start()
            stores.append(store)
    first = lax.axis_index("ba") * 2
    lane = lax.broadcasted_iota(jnp.int32, (4, N), 1)
    row = lax.broadcasted_iota(jnp.int32, (4, N), 0)
    start = lax.div(row, 2) * 16 + lax.rem(row, 2) + first
    whole = sums_ref[...]
    columns = [jnp.sum(jnp.where(lane == start + a * 4, whole, 0.0), axis=1, keepdims=True) for a in range(4)]
    gram = jnp.concatenate(columns, axis=1)
    gram_ref[0] = gram[:2]
    gram_ref[1] = gram[2:]
    for store in stores:
        store.wait()


def in_hbm(array):
    return pltpu.with_memory_space_constraint(array, pltpu.HBM)


def on_device(coeffs, material, inv_diag, inv_off):
    f32 = jnp.float32
    anywhere = pl.BlockSpec(memory_space=pltpu.HBM)
    vmem = pl.BlockSpec(memory_space=pltpu.VMEM)
    back, sums = pl.pallas_call(
        kernel,
        out_shape=(jax.ShapeDtypeStruct((6, 2 * N, 2 * N), f32), jax.ShapeDtypeStruct((1, N), f32)),
        in_specs=[anywhere] * 5,
        out_specs=(vmem, vmem),
        scratch_shapes=[
            pltpu.VMEM((2, 2, 3, 2, N, N), f32),
            pltpu.VMEM((2, N, N), jnp.int32),
            pltpu.SMEM((4, 3), f32),
            pltpu.SMEM((4, 3), f32),
            pltpu.VMEM((4, 2, 2 * N, 2 * N), jnp.bfloat16),
            pltpu.VMEM((CHUNKS, DEV * 8, N), f32),
            pltpu.VMEM((CHUNKS, DEV * 8, N), f32),
            pltpu.VMEM((6, 2 * N, 2 * N), f32),
            pltpu.VMEM((6, 2 * N, 2 * N), f32),
            pltpu.VMEM((CHUNKS, DEV * 8, N), f32),
            pltpu.VMEM((CHUNKS, DEV * 8, N), f32),
            pltpu.VMEM((DEV, 2, N), jnp.int32),
            pltpu.VMEM((GZ, 2, N), jnp.int32),
            pltpu.VMEM((6, N, N), f32),
            pltpu.VMEM((2, 1, N), f32),
            pltpu.VMEM((8, 1, N), f32),
            pltpu.VMEM((16, 1, N), f32),
            pltpu.SemaphoreType.DMA((6,)),
            pltpu.SemaphoreType.DMA((9,)),
            pltpu.SemaphoreType.DMA((10,)),
            pltpu.SemaphoreType.REGULAR((8,)),
        ],
        compiler_params=pltpu.CompilerParams(
            collective_id=0, has_side_effects=True, vmem_limit_bytes=32 * 1024 * 1024
        ),
        name="maxwell",
    )(in_hbm(coeffs), in_hbm(material), in_hbm(inv_diag), in_hbm(inv_off), in_hbm(jnp.asarray(tables())))
    theta, gram = pl.pallas_call(
        curl_kernel,
        out_shape=(jax.ShapeDtypeStruct(coeffs.shape, f32), jax.ShapeDtypeStruct((2, 2, 4), f32)),
        in_specs=[vmem, vmem],
        out_specs=(anywhere, vmem),
        scratch_shapes=[pltpu.VMEM((2, 2, 3, 2, N, N), f32), pltpu.SemaphoreType.DMA((4,))],
        compiler_params=pltpu.CompilerParams(vmem_limit_bytes=16 * 1024 * 1024),
        name="curl",
    )(back, sums)
    return theta, jnp.transpose(gram, (0, 2, 1))


def solution(mesh):
    in_specs = (P(None, None, "ba", "gz", None, None), P("gz", None, None), P(), P())
    out_specs = (P(None, None, "ba", "gz", None, None), P(None, None, "ba"))
    return jax.shard_map(
        on_device, mesh=mesh, in_specs=in_specs, out_specs=out_specs, check_vma=False
    )
```
